256 devices in a mesh: dom: 256 (over y, x, z, core).
Axes of the slice: x: 4, y: 4, z: 8, core: 2. Of those that a mesh axis runs over, the one named last changes fastest.
Arguments:
- right_side: float32 [8192, 16, 128], P('dom')
- band_blocks: float32 [8192, 5, 128, 128], P('dom'), as said below
- link_blocks: float32 [256, 6, 4, 128, 128], P('dom'), as said below
- link_rows: int32 [256, 6, 4], P('dom'), may hold values from 0 to 32, as said below
Outputs:
- solution: float32 [8192, 16, 128], P('dom')
- residual: float32 [8192, 16, 128], P('dom')
The draws below stay inside these ranges and needn't reach their ends.
Inputs may be any that keep to these rules, and one draw needn't show every extreme that they name: `link_rows`: entries are a row of device d (0 to 31) or 32 for an unused slot. Slot s of interface j of device d is paired with slot s of interface j xor 1 of the device it faces, and is used exactly when that one is. Each interface uses its first 1 to 4 slots and no row twice; in every draw some interface uses all 4. link_blocks[d, j, s] is the transpose of link_blocks[e, j xor 1, s] for the device e that interface j of d faces; blocks of unused slots are zero. band_blocks[g, 2 + m] is the transpose of band_blocks[g + m, 2 - m]; blocks whose column falls outside the device are zero. A is symmetric with a positive diagonal that exceeds the sum of magnitudes of the rest of its row.
All inputs are finite; a program needn't handle non-finite values.
Results may differ from the reference program's by a relative error of at most 0.0003.
Values sent between devices are 32-bit elements; how exact they have to be, the bound alone decides.
A program may use at most 64 MiB of HBM per device.

```python
import jax
import jax.numpy as jnp
from jax import lax

BS = 128
S = 16
R_DEV = 32
ITERS = 3
H = 4
NB = 8192
N_DOM = 256


def facing_offsets_drawn(dev_count):
    return (1, -1, dev_count // 16, -(dev_count // 16), dev_count // 4, -(dev_count // 4))


def rough_block(key, shape):
    weight = 1.0 / (7.0 * BS)
    spread = jax.random.uniform(key, shape, jnp.float32, 0.5, 1.5)
    return -weight * spread


def build_matrix(key):
    dev_count = N_DOM
    block_rows = R_DEV
    links = H
    offset_list = facing_offsets_drawn(dev_count)
    keys = jax.random.split(jax.random.fold_in(key, 11), 7)
    counts = jax.random.randint(keys[0], (dev_count, 3), 1, links + 1)
    fullest = jax.random.randint(keys[1], (3,), 0, dev_count)
    counts = counts.at[fullest, jnp.arange(3)].set(links)
    orders = jax.vmap(lambda sub: jax.random.permutation(sub, block_rows))(jax.random.split(keys[2], dev_count))
    slots = jnp.arange(links)
    used_list = []
    rows_list = []
    for facing in range(6):
        pair = facing // 2
        if facing % 2 == 0:
            owned = counts[:, pair]
        else:
            owned = jnp.roll(counts[:, pair], offset_list[facing - 1])
        used = slots[None, :] < owned[:, None]
        picked = orders[:, (facing * links + slots) % block_rows]
        used_list.append(used)
        rows_list.append(jnp.where(used, picked, block_rows).astype(jnp.int32))
    link_rows = jnp.stack(rows_list, axis=1)
    raw = rough_block(keys[3], (dev_count, 3, links, BS, BS))
    blocks_list = []
    for facing in range(6):
        pair = facing // 2
        kept = raw[:, pair] * used_list[2 * pair][:, :, None, None].astype(jnp.float32)
        if facing % 2 == 0:
            blocks_list.append(kept)
        else:
            blocks_list.append(jnp.roll(jnp.swapaxes(kept, -1, -2), offset_list[2 * pair], axis=0))
    link_blocks = jnp.stack(blocks_list, axis=1)
    upper = rough_block(keys[4], (dev_count, block_rows, 2, BS, BS))
    places = jnp.arange(block_rows)[:, None] + jnp.arange(1, 3)[None, :]
    upper = upper * (places < block_rows).astype(jnp.float32)[None, :, :, None, None]
    lower_one = jnp.swapaxes(jnp.roll(upper[:, :, 0], 1, axis=1), -1, -2)
    lower_two = jnp.swapaxes(jnp.roll(upper[:, :, 1], 2, axis=1), -1, -2)
    inner = rough_block(keys[5], (dev_count, block_rows, BS, BS))
    inner = 0.5 * (inner + jnp.swapaxes(inner, -1, -2))
    identity = jnp.eye(BS, dtype=jnp.float32)
    inner = inner * (1.0 - identity)
    row_abs = jnp.sum(jnp.abs(inner), axis=-1)
    row_abs = row_abs + jnp.sum(jnp.abs(upper), axis=(2, 4))
    row_abs = row_abs + jnp.sum(jnp.abs(lower_one), axis=-1) + jnp.sum(jnp.abs(lower_two), axis=-1)
    picks = (link_rows[:, :, :, None] == jnp.arange(block_rows)[None, None, None, :]).astype(jnp.float32)
    row_abs = row_abs + jnp.einsum('cjhr,cjhi->cri', picks, jnp.sum(jnp.abs(link_blocks), axis=-1))
    low, high = (0.05, 4.0)
    margin = jnp.exp(jax.random.uniform(keys[6], (dev_count, block_rows, BS), jnp.float32, jnp.log(low), jnp.log(high)))
    diagonal = inner + identity * (row_abs + margin)[..., :, None]
    band = jnp.stack([lower_two, lower_one, diagonal, upper[:, :, 0], upper[:, :, 1]], axis=2)
    return (link_rows, band.reshape(dev_count * block_rows, 5, BS, BS), link_blocks)


def draw_link_rows(key, part):
    return build_matrix(key)[0]


def draw_band_blocks(key, part):
    return build_matrix(key)[1]


def draw_link_blocks(key, part):
    return build_matrix(key)[2]


def draw_right_side(key, part):
    noise = jax.random.normal(jax.random.fold_in(key, 3), (NB, S, BS), jnp.float32)
    owner = (jnp.arange(NB) // R_DEV).astype(jnp.float32)
    rising = (1.0 + 2.0 * owner / (N_DOM - 1))[:, None, None]
    return noise * rising


def setup_inputs(seed: int = 0) -> dict:
    seeds = jax.random.split(jax.random.key(seed), 5)
    return {
        "right_side": draw_right_side(jax.random.fold_in(seeds[4], 71), 0),
        "band_blocks": draw_band_blocks(jax.random.fold_in(seeds[4], 71), 0),
        "link_blocks": draw_link_blocks(jax.random.fold_in(seeds[4], 71), 0),
        "link_rows": draw_link_rows(jax.random.fold_in(seeds[4], 71), 0),
    }


HIGHEST = lax.Precision.HIGHEST

def facing_offsets(dev_count):
    return (1, -1, dev_count // 16, -(dev_count // 16), dev_count // 4, -(dev_count // 4))

def apply_matrix(field, band_blocks, link_blocks, link_rows):
    dev_count = N_DOM
    block_rows = R_DEV
    shards = field.reshape(dev_count, block_rows, S, BS)
    padded = jnp.pad(shards, ((0, 0), (2, 2), (0, 0), (0, 0)))
    banded = band_blocks.reshape(dev_count, block_rows, 5, BS, BS)
    total = jnp.zeros_like(shards)
    for band_slot in range(5):
        total = total + jnp.einsum('nrsj,nrij->nrsi', padded[:, band_slot:band_slot + block_rows], banded[:, :, band_slot], precision=HIGHEST)
    extended = jnp.concatenate([shards, jnp.zeros((dev_count, 1, S, BS), field.dtype)], axis=1)
    devices = jnp.arange(dev_count, dtype=jnp.int32)
    offset_list = facing_offsets(dev_count)
    for facing in range(6):
        partner = ((devices + offset_list[facing]) % dev_count).astype(jnp.int32)
        far_rows = link_rows[partner, facing ^ 1]
        arrived = extended[partner[:, None], far_rows]
        contrib = jnp.einsum('nhsj,nhij->nhsi', arrived, link_blocks[:, facing], precision=HIGHEST)
        landing = jnp.zeros((dev_count, block_rows + 1, S, BS), field.dtype)
        landing = landing.at[devices[:, None], link_rows[:, facing]].add(contrib)
        total = total + landing[:, :block_rows]
    return total.reshape(NB, S, BS)

def gram_matrix(left, right):
    return jnp.einsum('nsi,nti->st', left, right, precision=HIGHEST)

def mix_columns(field, coeffs):
    return jnp.einsum('nsi,st->nti', field, coeffs, precision=HIGHEST)

def solve_gram(matrix, target):
    symmetric = 0.5 * (matrix + matrix.T)
    factor = jnp.linalg.cholesky(symmetric)
    return jax.scipy.linalg.cho_solve((factor, True), target)

def reference(right_side, band_blocks, link_blocks, link_rows):
    solution = jnp.zeros_like(right_side)
    residual = right_side
    direction = right_side
    squares = gram_matrix(residual, residual)
    for iteration in range(ITERS):
        image = apply_matrix(direction, band_blocks, link_blocks, link_rows)
        alpha = solve_gram(gram_matrix(direction, image), squares)
        solution = solution + mix_columns(direction, alpha)
        residual = residual - mix_columns(image, alpha)
        if iteration + 1 < ITERS:
            fresh = gram_matrix(residual, residual)
            beta = solve_gram(squares, fresh)
            direction = residual + mix_columns(direction, beta)
            squares = fresh
    return (solution, residual)
```

```python
import functools

import jax
import jax.numpy as jnp
from jax import lax
from jax.experimental import pallas as pl
from jax.experimental.pallas import tpu as pltpu
from jax.sharding import PartitionSpec as P

S = 16
BS = 128
W = 2 * BS
H = 4
MESH = pl.DeviceIdType.MESH
F32 = jnp.float32
BF16 = jnp.bfloat16


def dot(a, b):
    return jnp.dot(a, b, preferred_element_type=F32)


def dot_nt(a, b):
    return lax.dot_general(a, b, (((1,), (1,)), ((), ())), preferred_element_type=F32)


def split(x):
    hi = x.astype(BF16)
    return hi, (x - hi.astype(F32)).astype(BF16)


def halves(x):
    return x[:S] + x[S:]


def iota(shape, dim):
    return lax.broadcasted_iota(jnp.int32, shape, dim)


def eliminate(table, first, count):
    lane = iota((1, BS), 1)
    for k in range(count):
        col = table[:, first + k : first + k + 1]
        inverse = 1.0 / col[k : k + 1]
        row = table[k : k + 1] * inverse
        table = jnp.where(lane == first + k, col * inverse, table - col * row)
    return table


def kernel(
    n,
    zs,
    rhs,
    band,
    link,
    rows,
    x_out,
    r_out,
    v0,
    stage,
    lstage,
    tiles,
    links,
    vs,
    xs,
    vr,
    yb,
    w1,
    v2,
    inv,
    send,
    recv0,
    recv1,
    recv2,
    sig1,
    sig2,
    gra1,
    gra2,
    grb1,
    grb2,
    in_sem,
    band_sem,
    halo_send,
    halo_recv,
    s1,
    r1,
    s2,
    r2,
):
    block_rows = v0.shape[0]
    pairs = block_rows // 2
    group = n // zs
    me = lax.axis_index("dom")
    offsets = (1, n - 1, n // 16, n - n // 16, n // 4, n - n // 4)
    z = (me // 2) % zs
    rank = me // (2 * zs) * 2 + me % 2

    def plane_device(other):
        return other // 2 * (2 * zs) + z * 2 + other % 2

    def ring_device(other):
        return me - z * 2 + other * 2

    load_v = pltpu.make_async_copy(rhs, v0, in_sem.at[0])
    load_l = pltpu.make_async_copy(link.at[0], lstage, in_sem.at[1])
    load_v.start()
    load_l.start()

    def load_band(p):
        return pltpu.make_async_copy(band.at[pl.ds(2 * p, 2)], stage.at[pl.ds(2 * p, 2)], band_sem.at[p])

    @pl.loop(0, pairs)
    def _(p):
        load_band(p).start()

    barrier = pltpu.get_barrier_semaphore()
    for offset in offsets:
        pl.semaphore_signal(barrier, inc=1, device_id=((me + offset) % n,), device_id_type=MESH)

    @pl.loop(1, group)
    def _(i):
        pl.semaphore_signal(barrier, inc=1, device_id=(plane_device((rank + i) % group),), device_id_type=MESH)

    @pl.loop(1, zs)
    def _(i):
        pl.semaphore_signal(barrier, inc=1, device_id=(ring_device((z + i) % zs),), device_id_type=MESH)

    @pl.loop(0, block_rows)
    def _(g):
        for j in range(6):
            found = 0
            for s in range(H):
                found = jnp.where(rows[0, j, s] == g, s + 1, found)
            inv[g * 6 + j] = found

    zero_tile = jnp.zeros((6, S, BS), F32)
    for buffer in (recv0, recv1, recv2):
        buffer[:, 0] = zero_tile
    xs[:, pl.ds(0, W)] = jnp.zeros((2 * S, W), BF16)
    xs[:, pl.ds(W * (pairs + 1), W)] = jnp.zeros((2 * S, W), BF16)
    zero_block = jnp.zeros((BS, BS), BF16)

    @pl.loop(0, pairs)
    def _(q):
        for part in range(2):
            tiles[q + 1, pl.ds(part * 3 * W, BS), pl.ds(BS, BS)] = zero_block
            tiles[q + 1, pl.ds(part * 3 * W + 2 * W + BS, BS), pl.ds(0, BS)] = zero_block

    for part in range(2):
        tiles[1, pl.ds(part * 3 * W, W)] = jnp.zeros((W, W), BF16)
        tiles[pairs, pl.ds(part * 3 * W + 2 * W, W)] = jnp.zeros((W, W), BF16)

    def put(p, value, slots):
        hi, lo = split(value)
        both = jnp.concatenate([hi, lo], axis=0)
        xs[:, pl.ds(pl.multiple_of(W * (p + 1), W), W)] = both
        vr[2 * p] = both[:, :BS]
        vr[2 * p + 1] = both[:, BS:]
        if slots is not None:
            keep(p, slots, hi, lo)

    def keep(p, slot, hi, lo):
        lanes = pl.ds(pl.multiple_of(W * p, W), W)
        vs[pl.ds(S * slot, S), lanes] = hi
        vs[pl.ds(4 * S + S * slot, S), lanes] = lo

    def first_field(p):
        return jnp.concatenate([v0[2 * p], v0[2 * p + 1]], axis=1)

    load_v.wait()

    @pl.loop(0, pairs)
    def _(p):
        put(p, first_field(p), 0)

    load_l.wait()

    @pl.loop(0, 6)
    def _(j):
        for s in range(H):
            hi, lo = split(lstage[j, s])
            links[j, s, pl.ds(0, BS)] = hi
            links[j, s, pl.ds(BS, BS)] = lo

    def halo_copy(step, j):
        return pltpu.make_async_remote_copy(
            src_ref=send.at[step, j],
            dst_ref=(recv0, recv1, recv2)[step].at[j ^ 1, pl.ds(1, H)],
            send_sem=halo_send.at[step, j],
            recv_sem=halo_recv.at[step, j ^ 1],
            device_id=((me + offsets[j]) % n,),
            device_id_type=MESH,
        )

    def multiply_links(step, ready=None):
        for j in (2, 3, 4, 5, 0, 1):
            for s in range(H):
                mine = vr[jnp.minimum(rows[0, j, s], block_rows - 1)]
                send[step, j, s] = halves(dot(jnp.concatenate([mine, mine], axis=1), links[j, s]))
            if ready is None:
                halo_copy(step, j).start()

    multiply_links(0, ready=False)
    pl.semaphore_wait(barrier, 6 + group - 1 + zs - 1)
    for j in (2, 3, 4, 5, 0, 1):
        halo_copy(0, j).start()

    on_diagonal = iota((BS, BS), 0) == iota((BS, BS), 1)

    def split_pair(p, total):
        load_band(p).wait()
        for local in range(2):
            for slot in range(5):
                block = stage[2 * p + local, slot]
                if slot == 2:
                    total = total + jnp.sum(jnp.where(on_diagonal, block, 0.0), axis=0, keepdims=True)
                away = local + slot - 2
                q = away // 2
                hi, lo = split(block)
                at = (1 - q) * W + local * BS
                lanes = pl.ds((away % 2) * BS, BS)
                tiles[p + q + 1, pl.ds(at, BS), lanes] = hi
                tiles[p + q + 1, pl.ds(3 * W + at, BS), lanes] = lo
        return total

    diagonal = lax.fori_loop(0, pairs, split_pair, jnp.zeros((1, BS), F32))

    def plane_copy(which, buffer, i):
        other = (rank + i) % group
        return pltpu.make_async_remote_copy(
            src_ref=buffer.at[rank],
            dst_ref=buffer.at[rank],
            send_sem=s1.at[which, other],
            recv_sem=r1.at[which, rank],
            device_id=(plane_device(other),),
            device_id_type=MESH,
        )

    def ring_copy(which, buffer, i):
        other = (z + i) % zs
        return pltpu.make_async_remote_copy(
            src_ref=buffer.at[z],
            dst_ref=buffer.at[z],
            send_sem=s2.at[which, other],
            recv_sem=r2.at[which, z],
            device_id=(ring_device(other),),
            device_id_type=MESH,
        )

    def plane_start(which, buffer, value):
        buffer[rank] = value

        @pl.loop(1, group)
        def _(i):
            plane_copy(which, buffer, i).start()

    def plane_finish(which, buffer):
        @pl.loop(1, group)
        def _(i):
            other = (rank + i) % group
            pltpu.make_async_remote_copy(
                src_ref=buffer.at[other],
                dst_ref=buffer.at[other],
                send_sem=s1.at[which, other],
                recv_sem=r1.at[which, other],
                device_id=(plane_device(other),),
                device_id_type=MESH,
            ).wait_recv()

        return jnp.sum(buffer[...], axis=0)

    def ring_start(which, buffer, value):
        buffer[z] = value

        @pl.loop(1, zs)
        def _(i):
            ring_copy(which, buffer, i).start()

    def ring_finish(which, buffer):
        @pl.loop(1, zs)
        def _(i):
            other = (z + i) % zs
            pltpu.make_async_remote_copy(
                src_ref=buffer.at[other],
                dst_ref=buffer.at[other],
                send_sem=s2.at[which, other],
                recv_sem=r2.at[which, other],
                device_id=(ring_device(other),),
                device_id_type=MESH,
            ).wait_recv()

        return jnp.sum(buffer[...], axis=0)

    plane_start(0, sig1, diagonal * (1.0 / (block_rows * BS)))

    def band_product():
        def body(q, carry):
            lhs = xs[:, pl.ds(pl.multiple_of(W * q, W), 3 * W)]
            out = dot(lhs, tiles[q + 1, pl.ds(0, 3 * W)]) + dot(lhs, tiles[q + 1, pl.ds(3 * W, 3 * W)])
            yb[q] = halves(out)
            return carry

        lax.fori_loop(0, pairs, body, 0, unroll=True)

    def landed(buffer, p):
        def of_row(g):
            total = buffer[0, inv[g * 6]]
            for j in range(1, 6):
                total = total + buffer[j, inv[g * 6 + j]]
            return total

        return yb[p] + jnp.concatenate([of_row(2 * p), of_row(2 * p + 1)], axis=1)

    def wait_halo(step):
        for j in range(6):
            halo_copy(step, j).wait_recv()

    band_product()
    wait_halo(0)

    @pl.loop(0, pairs)
    def _(p):
        value = landed(recv0, p)
        w1[p] = value
        put(p, value, None)

    multiply_links(1)
    ring_start(0, sig2, plane_finish(0, sig1))
    band_product()
    wait_halo(1)
    sigma = jnp.sum(ring_finish(0, sig2), axis=1, keepdims=True) * (1.0 / n)
    scale = 1.0 / sigma

    @pl.loop(0, pairs)
    def _(p):
        first = w1[p]
        one = first * scale - first_field(p)
        keep(p, 1, *split(one))
        two = (landed(recv1, p) * scale - first) * scale - one
        v2[p] = two
        put(p, two, 2)

    multiply_links(2)
    low = vs[pl.ds(0, 3 * S)]
    high = vs[pl.ds(4 * S, 3 * S)]
    stack = jnp.concatenate([low, high], axis=0)
    grams = dot_nt(stack, stack)
    grams = grams[: 3 * S] + grams[3 * S :]
    grams = grams[:, : 3 * S] + grams[:, 3 * S :]

    def gram_of(a, b):
        return grams[S * a : S * a + S, S * b : S * b + S]

    packed = jnp.concatenate(
        [gram_of(0, 0), gram_of(0, 1), gram_of(1, 1), gram_of(1, 2), gram_of(2, 2), jnp.zeros((S, 3 * S), F32)], axis=1
    )
    plane_start(1, gra1, packed)
    band_product()
    wait_halo(2)

    @pl.loop(0, pairs)
    def _(p):
        value = landed(recv2, p) * scale - v2[p]
        keep(p, 3, *split(value))

    left = jnp.concatenate([vs[pl.ds(2 * S, S)], vs[pl.ds(6 * S, S)]], axis=0)
    right = jnp.concatenate([vs[pl.ds(3 * S, S)], vs[pl.ds(7 * S, S)]], axis=0)
    last = halves(dot_nt(left, right))
    last = last[:, :S] + last[:, S:]
    lane = iota((S, BS), 1)
    place = lane // S == iota((S, BS), 0) % 8
    spread = jnp.where(place, jnp.concatenate([last] * 8, axis=1), 0.0)
    plane_start(2, grb1, jnp.concatenate([jnp.sum(spread[:8], axis=0, keepdims=True), jnp.sum(spread[8:], axis=0, keepdims=True)], axis=0))
    ring_start(1, gra2, plane_finish(1, gra1))
    ring_start(2, grb2, plane_finish(2, grb1))
    moments = ring_finish(1, gra2)

    in_h = lane < 3 * S
    blocks = []
    for i in range(3):
        upper = pltpu.roll(moments, BS - S * (i + 1), 1)
        lower = moments if i == 0 else pltpu.roll(moments, BS - S * i, 1)
        blocks.append(jnp.where(in_h, upper + lower, 0.0))
    blocks.append(jnp.where(in_h, moments, 0.0))
    table = jnp.concatenate(blocks, axis=0)
    table = eliminate(table, 0, S)[S:]
    table = eliminate(table, S, S)[S:]
    late = ring_finish(2, grb2)
    spread = jnp.concatenate([jnp.broadcast_to(late[:1], (8, BS)), jnp.broadcast_to(late[1:], (8, BS))], axis=0)
    spread = jnp.where(place, spread, 0.0)
    for shift in (64, 32, 16):
        spread = spread + pltpu.roll(spread, shift, 1)
    spread = jnp.where((lane >= 2 * S) & (lane < 3 * S), spread, 0.0)
    table = jnp.concatenate([table[:S] + spread, table[S:]], axis=0)
    coeffs = eliminate(table, 2 * S, S)[S:]
    coeffs = jnp.where(in_h, coeffs, 0.0)

    of_x = coeffs * scale
    of_r = -(coeffs + pltpu.roll(coeffs, S, 1))
    both = jnp.concatenate([of_x, of_r], axis=0)
    both = both + pltpu.roll(both, 4 * S, 1)
    hi, lo = split(both)
    mixer = jnp.concatenate([hi, lo], axis=0)

    def mix(p, carry):
        out = dot(mixer, vs[:, pl.ds(pl.multiple_of(W * p, W), W)])
        out = out[: 2 * S] + out[2 * S :]
        for local in range(2):
            lanes = slice(BS * local, BS * local + BS)
            x_out[2 * p + local] = out[:S, lanes]
            r_out[2 * p + local] = v0[2 * p + local] + out[S:, lanes]
        return carry

    lax.fori_loop(0, pairs, mix, 0, unroll=True)

    for step in range(3):
        for j in range(6):
            halo_copy(step, j).wait_send()
    for which, plane, ring in ((0, sig1, sig2), (1, gra1, gra2), (2, grb1, grb2)):

        @pl.loop(1, group)
        def _(i):
            plane_copy(which, plane, i).wait_send()

        @pl.loop(1, zs)
        def _(i):
            ring_copy(which, ring, i).wait_send()


def solution(mesh):
    n = mesh.devices.size
    zs = max(n // 32, 2)
    group = n // zs

    def local(right_side, band_blocks, link_blocks, link_rows):
        block_rows = right_side.shape[0]
        pairs = block_rows // 2
        field = jax.ShapeDtypeStruct(right_side.shape, F32)
        vmem = pltpu.VMEM
        dma = pltpu.SemaphoreType.DMA
        hbm = pl.BlockSpec(memory_space=pl.ANY)
        return pl.pallas_call(
            functools.partial(kernel, n, zs),
            out_shape=(field, field),
            in_specs=[hbm, hbm, hbm, pl.BlockSpec(memory_space=pltpu.SMEM)],
            out_specs=(pl.BlockSpec(memory_space=pltpu.VMEM),) * 2,
            scratch_shapes=[
                vmem((block_rows, S, BS), F32),
                vmem((block_rows, 5, BS, BS), F32),
                vmem((6, H, BS, BS), F32),
                vmem((pairs + 2, 6 * W, W), BF16),
                vmem((6, H, W, BS), BF16),
                vmem((8 * S, W * pairs), BF16),
                vmem((2 * S, W * (pairs + 2)), BF16),
                vmem((block_rows, 2 * S, BS), BF16),
                vmem((pairs, S, W), F32),
                vmem((pairs, S, W), F32),
                vmem((pairs, S, W), F32),
                pltpu.SMEM((block_rows * 6,), jnp.int32),
                vmem((3, 6, H, S, BS), F32),
                vmem((6, H + 1, S, BS), F32),
                vmem((6, H + 1, S, BS), F32),
                vmem((6, H + 1, S, BS), F32),
                vmem((group, 1, BS), F32),
                vmem((zs, 1, BS), F32),
                vmem((group, S, BS), F32),
                vmem((zs, S, BS), F32),
                vmem((group, 2, BS), F32),
                vmem((zs, 2, BS), F32),
                dma((2,)),
                dma((pairs,)),
                dma((3, 6)),
                dma((3, 6)),
                dma((3, group)),
                dma((3, group)),
                dma((3, zs)),
                dma((3, zs)),
            ],
            compiler_params=pltpu.CompilerParams(
                collective_id=0, has_side_effects=True, vmem_limit_bytes=56 * 1024 * 1024
            ),
        )(right_side, band_blocks, link_blocks, link_rows)

    return jax.shard_map(
        local,
        mesh=mesh,
        in_specs=(P("dom", None, None), P("dom", None, None, None), P("dom", None, None, None, None), P("dom", None, None)),
        out_specs=(P("dom", None, None), P("dom", None, None)),
        check_vma=False,
    )
```

```python
import functools

import jax
import jax.numpy as jnp
from jax import lax
from jax.experimental import pallas as pl
from jax.experimental.pallas import tpu as pltpu
from jax.sharding import PartitionSpec as P

S = 16
BS = 128
W = 2 * BS
H = 4
MESH = pl.DeviceIdType.MESH
F32 = jnp.float32
BF16 = jnp.bfloat16


def dot(a, b):
    return jnp.dot(a, b, preferred_element_type=F32)


def dot_nt(a, b):
    return lax.dot_general(a, b, (((1,), (1,)), ((), ())), preferred_element_type=F32)


def split(x):
    hi = x.astype(BF16)
    return hi, (x - hi.astype(F32)).astype(BF16)


def halves(x):
    return x[:S] + x[S:]


def iota(shape, dim):
    return lax.broadcasted_iota(jnp.int32, shape, dim)


def eliminate(table, first, count):
    lane = iota((1, BS), 1)
    for k in range(count):
        col = table[:, first + k : first + k + 1]
        inverse = 1.0 / col[k : k + 1]
        row = table[k : k + 1] * inverse
        table = jnp.where(lane == first + k, col * inverse, table - col * row)
    return table


def eliminate_columns(upper, lower):
    count = len(upper)
    for k in range(count):
        inverse = 1.0 / upper[k][k : k + 1]
        up, low = upper[k] * inverse, lower[k] * inverse
        for j in range(count):
            if j != k:
                factor = upper[j][k : k + 1]
                upper[j], lower[j] = upper[j] - up * factor, lower[j] - low * factor
        upper[k], lower[k] = up, low
    return lower


def pack(gram, place):
    spread = jnp.where(place, jnp.concatenate([gram] * 8, axis=1), 0.0)
    return jnp.concatenate(
        [jnp.sum(spread[:8], axis=0, keepdims=True), jnp.sum(spread[8:], axis=0, keepdims=True)], axis=0
    )


def widen(packed):
    return jnp.concatenate(
        [jnp.broadcast_to(packed[:1], (8, BS)), jnp.broadcast_to(packed[1:], (8, BS))], axis=0
    )


def unpack(packed, place):
    spread = jnp.where(place, widen(packed), 0.0)
    for shift in (64, 32, 16):
        spread = spread + pltpu.roll(spread, shift, 1)
    return spread


def kernel(
    n,
    zs,
    rhs,
    band,
    link,
    rows_in,
    x_out,
    r_out,
    rows,
    v0,
    stage,
    lstage,
    tiles,
    links,
    vs,
    xs,
    vr,
    yb,
    ys,
    w1,
    v2,
    inv,
    send,
    recv0,
    recv1,
    recv2,
    sig1,
    sig2,
    gra1,
    gra2,
    grb1,
    grb2,
    in_sem,
    band_sem,
    halo_send,
    halo_recv,
    s1,
    r1,
    s2,
    r2,
):
    block_rows = v0.shape[0]
    pairs = block_rows // 2
    group = n // zs
    me = lax.axis_index("dom")
    offsets = (1, n - 1, n // 16, n - n // 16, n // 4, n - n // 4)
    z = lax.rem(lax.div(me, 2), zs)
    rank = lax.div(me, 2 * zs) * 2 + lax.rem(me, 2)

    def plane_device(other):
        return lax.div(other, 2) * (2 * zs) + z * 2 + lax.rem(other, 2)

    def ring_device(other):
        return me - z * 2 + other * 2

    barrier = pltpu.get_barrier_semaphore()
    with jax.named_scope("signals"):
        for i in range(1, group):
            device = plane_device(lax.rem(rank + i, group))
            pl.semaphore_signal(barrier, inc=1, device_id=(device,), device_id_type=MESH)
        for i in range(1, zs):
            device = ring_device(lax.rem(z + i, zs))
            pl.semaphore_signal(barrier, inc=1, device_id=(device,), device_id_type=MESH)
        for offset in offsets:
            device = lax.rem(me + offset, n)
            pl.semaphore_signal(barrier, inc=1, device_id=(device,), device_id_type=MESH)

    load_r = pltpu.make_async_copy(rows_in, rows, in_sem.at[0])
    load_v = pltpu.make_async_copy(rhs, v0, in_sem.at[1])
    load_l = pltpu.make_async_copy(link.at[0], lstage, in_sem.at[2])
    load_d = pltpu.make_async_copy(band.at[:, 2], stage.at[:, 2], in_sem.at[3])

    def load_band(p, side):
        at = (pl.ds(2 * p, 2), pl.ds(3 * side, 2))
        return pltpu.make_async_copy(band.at[at], stage.at[at], band_sem.at[p, side])

    with jax.named_scope("starts"):
        load_r.start()
        load_v.start()
        load_l.start()
        load_d.start()
        for p in range(pairs):
            load_band(p, 0).start()
            load_band(p, 1).start()

    with jax.named_scope("zeros"):
        for buffer in (recv0, recv1, recv2):
            buffer[:, 0] = jnp.zeros((6, S, BS), F32)
        xs[:, pl.ds(0, W)] = jnp.zeros((2 * S, W), BF16)
        xs[:, pl.ds(W * (pairs + 1), W)] = jnp.zeros((2 * S, W), BF16)
        zero_block = jnp.zeros((BS, BS), BF16)

        @pl.loop(0, pairs)
        def _(q):
            for part in range(2):
                tiles[q + 1, pl.ds(part * 3 * W, BS), pl.ds(BS, BS)] = zero_block
                tiles[q + 1, pl.ds(part * 3 * W + 2 * W + BS, BS), pl.ds(0, BS)] = zero_block

        for part in range(2):
            tiles[1, pl.ds(part * 3 * W, W)] = jnp.zeros((W, W), BF16)
            tiles[pairs, pl.ds(part * 3 * W + 2 * W, W)] = jnp.zeros((W, W), BF16)

    def each_pair(body):
        def step(p, carry):
            body(p)
            return carry

        lax.fori_loop(0, pairs, step, 0, unroll=True)

    def put(p, value, slot):
        hi, lo = split(value)
        both = jnp.concatenate([hi, lo], axis=0)
        xs[:, pl.ds(pl.multiple_of(W * (p + 1), W), W)] = both
        vr[2 * p] = both[:, :BS]
        vr[2 * p + 1] = both[:, BS:]
        if slot is not None:
            keep(p, slot, hi, lo)

    def keep(p, slot, hi, lo):
        lanes = pl.ds(pl.multiple_of(W * p, W), W)
        vs[pl.ds(S * slot, S), lanes] = hi
        vs[pl.ds(4 * S + S * slot, S), lanes] = lo

    def first_field(p):
        return jnp.concatenate([v0[2 * p], v0[2 * p + 1]], axis=1)

    with jax.named_scope("inv"):
        load_r.wait()
        at = [[rows[0, s, j] for s in range(H)] for j in range(6)]

        @pl.loop(0, block_rows)
        def _(g):
            for j in range(6):
                found = 0
                for s in range(H):
                    found = jnp.where(at[j][s] == g, s + 1, found)
                inv[g * 6 + j] = found

    with jax.named_scope("load_v"):
        load_v.wait()
        each_pair(lambda p: put(p, first_field(p), 0))

    with jax.named_scope("load_l"):
        load_l.wait()
        for j in range(6):
            for s in range(H):
                hi, lo = split(lstage[j, s])
                links[j, s, pl.ds(0, BS)] = hi
                links[j, s, pl.ds(BS, BS)] = lo

    def halo_copy(step, j):
        return pltpu.make_async_remote_copy(
            src_ref=send.at[step, j],
            dst_ref=(recv0, recv1, recv2)[step].at[j ^ 1, pl.ds(1, H)],
            send_sem=halo_send.at[step, j],
            recv_sem=halo_recv.at[step, j ^ 1],
            device_id=(lax.rem(me + offsets[j], n),),
            device_id_type=MESH,
        )

    def row_of(j, s):
        return vr[jnp.minimum(rows[0, s, j], block_rows - 1)]

    def multiply_links(step):
        for j in range(6):
            for s in range(H):
                mine = row_of(j, s)
                send[step, j, s] = halves(dot(jnp.concatenate([mine, mine], axis=1), links[j, s]))

    def send_links(step):
        for j in (0, 1, 2, 3, 4, 5):
            halo_copy(step, j).start()

    with jax.named_scope("links0"):
        multiply_links(0)

    def plane_copy(which, buffer, i):
        other = lax.rem(rank + i, group)
        return pltpu.make_async_remote_copy(
            src_ref=buffer.at[rank],
            dst_ref=buffer.at[rank],
            send_sem=s1.at[which, other],
            recv_sem=r1.at[which, rank],
            device_id=(plane_device(other),),
            device_id_type=MESH,
        )

    def ring_copy(which, buffer, i):
        other = lax.rem(z + i, zs)
        return pltpu.make_async_remote_copy(
            src_ref=buffer.at[z],
            dst_ref=buffer.at[z],
            send_sem=s2.at[which, other],
            recv_sem=r2.at[which, z],
            device_id=(ring_device(other),),
            device_id_type=MESH,
        )

    def times(count, body):
        def step(i, carry):
            body(i)
            return carry

        lax.fori_loop(1, count, step, 0, unroll=True)

    def plane_start(which, buffer, value):
        buffer[rank] = value
        times(group, lambda i: plane_copy(which, buffer, i).start())

    def plane_finish(which, buffer):
        def wait(i):
            other = lax.rem(rank + i, group)
            pltpu.make_async_remote_copy(
                src_ref=buffer.at[other],
                dst_ref=buffer.at[other],
                send_sem=s1.at[which, other],
                recv_sem=r1.at[which, other],
                device_id=(plane_device(other),),
                device_id_type=MESH,
            ).wait_recv()

        times(group, wait)
        return jnp.sum(buffer[...], axis=0)

    def ring_start(which, buffer, value):
        buffer[z] = value
        times(zs, lambda i: ring_copy(which, buffer, i).start())

    def ring_finish(which, buffer):
        def wait(i):
            other = lax.rem(z + i, zs)
            pltpu.make_async_remote_copy(
                src_ref=buffer.at[other],
                dst_ref=buffer.at[other],
                send_sem=s2.at[which, other],
                recv_sem=r2.at[which, other],
                device_id=(ring_device(other),),
                device_id_type=MESH,
            ).wait_recv()

        times(zs, wait)
        return jnp.sum(buffer[...], axis=0)

    def plane_sent(which, buffer):
        times(group, lambda i: plane_copy(which, buffer, i).wait_send())

    def ring_sent(which, buffer):
        times(zs, lambda i: ring_copy(which, buffer, i).wait_send())

    with jax.named_scope("diagonal"):
        load_d.wait()
        on_diagonal = iota((BS, BS), 0) == iota((BS, BS), 1)

        def add_diagonal(g, total):
            return total + jnp.where(on_diagonal, stage[g, 2], 0.0)

        total = lax.fori_loop(0, block_rows, add_diagonal, jnp.zeros((BS, BS), F32), unroll=4)
        mean = jnp.sum(total * (1.0 / (block_rows * BS)), axis=0, keepdims=True)

    with jax.named_scope("barrier_wait"):
        pl.semaphore_wait(barrier, 6 + group - 1 + zs - 1)
    with jax.named_scope("send0"):
        send_links(0)
        plane_start(0, sig1, mean)

    with jax.named_scope("split_band"):

        @pl.loop(0, pairs)
        def _(p):
            load_band(p, 0).wait()
            load_band(p, 1).wait()
            for local in range(2):
                for slot in range(5):
                    away = local + slot - 2
                    q = away // 2
                    hi, lo = split(stage[2 * p + local, slot])
                    top = (1 - q) * W + local * BS
                    lanes = pl.ds((away % 2) * BS, BS)
                    tiles[p + q + 1, pl.ds(top, BS), lanes] = hi
                    tiles[p + q + 1, pl.ds(3 * W + top, BS), lanes] = lo

    def band_product():
        def body(q):
            lhs = xs[:, pl.ds(pl.multiple_of(W * q, W), 3 * W)]
            out = dot(lhs, tiles[q + 1, pl.ds(0, 3 * W)]) + dot(lhs, tiles[q + 1, pl.ds(3 * W, 3 * W)])
            yb[q] = halves(out)

        each_pair(body)

    def landed(buffer, p):
        def of_row(g):
            total = buffer[0, inv[g * 6]]
            for j in range(1, 6):
                total = total + buffer[j, inv[g * 6 + j]]
            return total

        return yb[p] + jnp.concatenate([of_row(2 * p), of_row(2 * p + 1)], axis=1)

    def wait_halo(step):
        for j in range(6):
            halo_copy(step, j).wait_recv()

    with jax.named_scope("band0"):
        band_product()
    with jax.named_scope("halo0"):
        wait_halo(0)

    def store_w1(p):
        value = landed(recv0, p)
        w1[p] = value
        put(p, value, None)

    with jax.named_scope("land0"):
        each_pair(store_w1)

    with jax.named_scope("links1"):
        multiply_links(1)
        send_links(1)
    with jax.named_scope("sig_ring"):
        ring_start(0, sig2, plane_finish(0, sig1))
    with jax.named_scope("band1"):
        band_product()
    with jax.named_scope("halo1"):
        wait_halo(1)
    with jax.named_scope("sig_wait"):
        sigma = jnp.sum(ring_finish(0, sig2) * (1.0 / n), axis=1, keepdims=True)
        scale = 1.0 / sigma

    def store_v2(p):
        first = w1[p]
        one = first * scale - first_field(p)
        keep(p, 1, *split(one))
        two = (landed(recv1, p) * scale - first) * scale - one
        v2[p] = two
        put(p, two, 2)

    with jax.named_scope("land1"):
        each_pair(store_v2)

    with jax.named_scope("links2"):
        multiply_links(2)
        send_links(2)
    lane = iota((S, BS), 1)
    place = lax.div(lane, S) == lax.rem(iota((S, BS), 0), 8)
    with jax.named_scope("grams"):
        stack = jnp.concatenate([vs[pl.ds(0, 3 * S)], vs[pl.ds(4 * S, 3 * S)]], axis=0)
        grams = dot_nt(stack, stack)
        grams = grams[: 3 * S] + grams[3 * S :]
        grams = grams[:, : 3 * S] + grams[:, 3 * S :]

        def gram_of(a, b):
            return grams[S * a : S * a + S, S * b : S * b + S]

        pairs_of = ((0, 0), (0, 1), (1, 1), (1, 2), (2, 2))
        plane_start(1, gra1, jnp.stack([pack(gram_of(a, b), place) for a, b in pairs_of]))
    with jax.named_scope("band2"):
        band_product()

        def split_y(p):
            hi, lo = split(yb[p])
            ys[:, pl.ds(pl.multiple_of(W * p, W), W)] = jnp.concatenate([hi, lo], axis=0)

        each_pair(split_y)
    with jax.named_scope("gram_y"):
        field = jnp.concatenate([vs[pl.ds(2 * S, S)], vs[pl.ds(6 * S, S)]], axis=0)
        partial = halves(dot_nt(field, ys[pl.ds(0, S)]) + dot_nt(field, ys[pl.ds(S, S)]))
        partial = partial * scale - gram_of(2, 2)
        slots = [(j, s) for j in range(6) for s in range(H)]
        mine = jnp.concatenate([row_of(j, s) for j, s in slots], axis=1)
    with jax.named_scope("halo2"):
        wait_halo(2)
    with jax.named_scope("gram_c"):
        came = [split(recv2[j, s + 1]) for j, s in slots]
        arrived = dot_nt(mine, jnp.concatenate([hi for hi, _ in came], axis=1))
        arrived = arrived + dot_nt(mine, jnp.concatenate([lo for _, lo in came], axis=1))
        last = partial + halves(arrived) * scale
        plane_start(2, grb1, pack(last, place))

    def store_v3(p):
        keep(p, 3, *split(landed(recv2, p) * scale - v2[p]))

    with jax.named_scope("land2"):
        each_pair(store_v3)
    with jax.named_scope("gra_plane"):
        ring_start(1, gra2, plane_finish(1, gra1))
    with jax.named_scope("sent"):
        for step in range(3):
            for j in range(6):
                halo_copy(step, j).wait_send()
        plane_sent(0, sig1)
        ring_sent(0, sig2)
        plane_sent(1, gra1)
    with jax.named_scope("grb_plane"):
        ring_start(2, grb2, plane_finish(2, grb1))
    with jax.named_scope("gra_ring"):
        moments = ring_finish(1, gra2)

    with jax.named_scope("early"):
        m = [unpack(moments[k], place) for k in range(5)]

        def across(parts):
            total = jnp.where(lane < S, parts[0], 0.0)
            for k in (1, 2):
                total = jnp.where((lane >= S * k) & (lane < S * (k + 1)), parts[k], total)
            return total

        table = jnp.concatenate(
            [
                across([m[1] + m[0], m[2] + m[1], m[3] + m[2]]),
                across([m[2] + m[1], m[3] + m[2], m[4] + m[3]]),
                across([m[3] + m[2], m[4] + m[3], m[4]]),
                across([m[0], m[1], m[2]]),
            ],
            axis=0,
        )
        table = eliminate(table, 0, S)[S:]
        table = eliminate(table, S, S)[S:]
        middle, right = table[:S], table[S:]
        early = lane < 2 * S
        gain = jnp.where(early, middle, jnp.where(lane == 2 * S + iota((S, BS), 0), -1.0, 0.0))
        base = jnp.where(early, right, 0.0)

        def of_outputs(coeffs):
            both = jnp.concatenate([coeffs * scale, -(coeffs + pltpu.roll(coeffs, S, 1))], axis=0)
            return both + pltpu.roll(both, 4 * S, 1)

        gain, base = of_outputs(gain), of_outputs(base)
        upper = [jnp.broadcast_to(middle[:, 2 * S + j : 2 * S + j + 1], (S, BS)) for j in range(S)]
        lower = [jnp.broadcast_to(right[:, 2 * S + j : 2 * S + j + 1], (S, BS)) for j in range(S)]
        from_lane = lax.rem(iota((S, BS), 0), 8) * S
        plane_sent(2, grb1)
        ring_sent(1, gra2)

    with jax.named_scope("grb_ring"):
        late = ring_finish(2, grb2)
    with jax.named_scope("late"):
        late = widen(late)
        for j in range(S):
            upper[j] = upper[j] + jnp.sum(jnp.where(lane == from_lane + j, late, 0.0), axis=1, keepdims=True)
        columns = eliminate_columns(upper, lower)
        both = base
        for j in range(S):
            both = both - jnp.concatenate(
                [columns[j] * gain[j : j + 1], columns[j] * gain[S + j : S + j + 1]], axis=0
            )
        hi, lo = split(both)
        mixer = jnp.concatenate([hi, lo], axis=0)

    def mix(p):
        out = dot(mixer, vs[:, pl.ds(pl.multiple_of(W * p, W), W)])
        out = out[: 2 * S] + out[2 * S :]
        for local in range(2):
            lanes = slice(BS * local, BS * local + BS)
            x_out[2 * p + local] = out[:S, lanes]
            r_out[2 * p + local] = v0[2 * p + local] + out[S:, lanes]

    with jax.named_scope("mix"):
        each_pair(mix)
    with jax.named_scope("tail"):
        ring_sent(2, grb2)


def write_out(x, r, x_out, r_out, sem):
    copies = [pltpu.make_async_copy(x, x_out, sem.at[0]), pltpu.make_async_copy(r, r_out, sem.at[1])]
    for copy in copies:
        copy.start()
    for copy in copies:
        copy.wait()


def solution(mesh):
    n = mesh.devices.size
    zs = max(n // 32, 2)
    group = n // zs

    def local(right_side, band_blocks, link_blocks, link_rows):
        block_rows = right_side.shape[0]
        pairs = block_rows // 2
        field = jax.ShapeDtypeStruct(right_side.shape, F32)
        vmem = pltpu.VMEM
        dma = pltpu.SemaphoreType.DMA
        hbm = pl.BlockSpec(memory_space=pl.ANY)
        local_vmem = pl.BlockSpec(memory_space=pltpu.VMEM)
        outs = pl.pallas_call(
            functools.partial(kernel, n, zs),
            out_shape=(pltpu.VMEM(right_side.shape, F32),) * 2,
            in_specs=[pl.BlockSpec(memory_space=pltpu.HBM)] * 4,
            out_specs=(local_vmem,) * 2,
            scratch_shapes=[
                pltpu.SMEM((1, H, 6), jnp.int32),
                vmem((block_rows, S, BS), F32),
                vmem((block_rows, 5, BS, BS), F32),
                vmem((6, H, BS, BS), F32),
                vmem((pairs + 2, 6 * W, W), BF16),
                vmem((6, H, W, BS), BF16),
                vmem((8 * S, W * pairs), BF16),
                vmem((2 * S, W * (pairs + 2)), BF16),
                vmem((block_rows, 2 * S, BS), BF16),
                vmem((pairs, S, W), F32),
                vmem((2 * S, W * pairs), BF16),
                vmem((pairs, S, W), F32),
                vmem((pairs, S, W), F32),
                pltpu.SMEM((block_rows * 6,), jnp.int32),
                vmem((3, 6, H, S, BS), F32),
                vmem((6, H + 1, S, BS), F32),
                vmem((6, H + 1, S, BS), F32),
                vmem((6, H + 1, S, BS), F32),
                vmem((group, 1, BS), F32),
                vmem((zs, 1, BS), F32),
                vmem((group, 5, 2, BS), F32),
                vmem((zs, 5, 2, BS), F32),
                vmem((group, 2, BS), F32),
                vmem((zs, 2, BS), F32),
                dma((4,)),
                dma((pairs, 2)),
                dma((3, 6)),
                dma((3, 6)),
                dma((3, group)),
                dma((3, group)),
                dma((3, zs)),
                dma((3, zs)),
            ],
            compiler_params=pltpu.CompilerParams(
                collective_id=0, has_side_effects=True, vmem_limit_bytes=64904 * 1024
            ),
        )(
            *(
                pltpu.with_memory_space_constraint(x, pltpu.HBM)
                for x in (right_side, band_blocks, link_blocks, jnp.transpose(link_rows, (0, 2, 1)))
            )
        )
        return pl.pallas_call(
            write_out,
            out_shape=(field, field),
            in_specs=[local_vmem] * 2,
            out_specs=(hbm, hbm),
            scratch_shapes=[dma((2,))],
        )(*(pltpu.with_memory_space_constraint(o, pltpu.VMEM) for o in outs))

    return jax.shard_map(
        local,
        mesh=mesh,
        in_specs=(P("dom", None, None), P("dom", None, None, None), P("dom", None, None, None, None), P("dom", None, None)),
        out_specs=(P("dom", None, None), P("dom", None, None)),
        check_vma=False,
    )
```

```python
import functools

import jax
import jax.numpy as jnp
from jax import lax
from jax.experimental import pallas as pl
from jax.experimental.pallas import tpu as pltpu
from jax.sharding import PartitionSpec as P

S = 16
BS = 128
W = 2 * BS
H = 4
MESH = pl.DeviceIdType.MESH
F32 = jnp.float32
BF16 = jnp.bfloat16


def dot(a, b):
    return jnp.dot(a, b, preferred_element_type=F32)


def dot_nt(a, b):
    return lax.dot_general(a, b, (((1,), (1,)), ((), ())), preferred_element_type=F32)


def split(x):
    hi = x.astype(BF16)
    return hi, (x - hi.astype(F32)).astype(BF16)


def halves(x):
    return x[:S] + x[S:]


def iota(shape, dim):
    return lax.broadcasted_iota(jnp.int32, shape, dim)


def eliminate(upper, lower):
    count = len(upper)
    for k in range(count):
        inverse = 1.0 / upper[k][k : k + 1]
        up, low = upper[k] * inverse, lower[k] * inverse
        for j in range(count):
            if j != k:
                factor = upper[j][k : k + 1]
                upper[j], lower[j] = upper[j] - up * factor, lower[j] - low * factor
        upper[k], lower[k] = up, low
    return lower


def sweep(table, first):
    lane = iota((S, BS), 1)
    rows = table.shape[0] - S

    def spread(part, k, height):
        return jnp.broadcast_to(part[:, first + k : first + k + 1], (height, BS))

    top, rest = table[:S], table[S:]
    columns = eliminate([spread(top, k, S) for k in range(S)], [spread(rest, k, rows) for k in range(S)])
    mine = (lane >= first) & (lane < first + S)
    top = jnp.where(lane == first + iota((S, BS), 0), -1.0, jnp.where(mine, 0.0, top))
    lane = iota((1, BS), 1)
    rest = jnp.where((lane >= first) & (lane < first + S), 0.0, rest)
    for k in range(S):
        rest = rest - columns[k] * top[k : k + 1]
    return rest


def pack(gram, place):
    spread = jnp.where(place, jnp.concatenate([gram] * 8, axis=1), 0.0)
    return jnp.concatenate(
        [jnp.sum(spread[:8], axis=0, keepdims=True), jnp.sum(spread[8:], axis=0, keepdims=True)], axis=0
    )


def widen(packed):
    return jnp.concatenate(
        [jnp.broadcast_to(packed[:1], (8, BS)), jnp.broadcast_to(packed[1:], (8, BS))], axis=0
    )


def unpack(packed, place):
    spread = jnp.where(place, widen(packed), 0.0)
    for shift in (64, 32, 16):
        spread = spread + pltpu.roll(spread, shift, 1)
    return spread


def kernel(
    n,
    zs,
    rhs,
    band,
    link,
    rows_in,
    v0,
    vs,
    mixer_out,
    rows,
    stage,
    lstage,
    tiles,
    links,
    xs,
    vr,
    yb,
    ys,
    w1,
    v2,
    inv,
    send,
    recv0,
    recv1,
    recv2,
    sig1,
    sig2,
    gra1,
    gra2,
    grb1,
    grb2,
    in_sem,
    band_sem,
    halo_send,
    halo_recv,
    s1,
    r1,
    s2,
    r2,
):
    block_rows = v0.shape[0]
    pairs = block_rows // 2
    group = n // zs
    me = lax.axis_index("dom")
    offsets = (1, n - 1, n // 16, n - n // 16, n // 4, n - n // 4)
    z = lax.rem(lax.div(me, 2), zs)
    rank = lax.div(me, 2 * zs) * 2 + lax.rem(me, 2)

    def hops(i):
        return sum((0, 1, 2, 1)[i >> at & 3] for at in (1, 3))

    plane_masks = [i // 2 * 2 * zs + i % 2 for i in sorted(range(1, group), key=hops, reverse=True)]
    ring_masks = [2 * i for i in sorted(range(1, zs), key=(0, 1, 3, 2, 7, 6, 5, 4).index if zs == 8 else None, reverse=True)]

    barrier = pltpu.get_barrier_semaphore()

    def announce(device):
        pl.semaphore_signal(barrier, inc=1, device_id=(device,), device_id_type=MESH)

    load_r = pltpu.make_async_copy(rows_in, rows, in_sem.at[0])
    load_v = pltpu.make_async_copy(rhs, v0, in_sem.at[1])
    load_l = pltpu.make_async_copy(link.at[0], lstage, in_sem.at[2])
    load_d = pltpu.make_async_copy(band.at[:, 2], stage.at[:, 2], in_sem.at[3])
    quarter = pairs // 4

    def load_band(c, side):
        at = (pl.ds(2 * quarter * c, 2 * quarter), pl.ds(3 * side, 2))
        return pltpu.make_async_copy(band.at[at], stage.at[at], band_sem.at[c, side])

    with jax.named_scope("signals"):
        for offset in offsets:
            announce(lax.rem(me + offset, n))
        load_r.start()
        load_v.start()
        load_l.start()
        load_d.start()
        for c in range(4):
            load_band(c, 0).start()
            load_band(c, 1).start()
        for mask in ring_masks + plane_masks:
            announce(me ^ mask)

    with jax.named_scope("zeros"):
        for buffer in (recv0, recv1, recv2):
            buffer[:, 0] = jnp.zeros((6, S, BS), F32)
        xs[:, pl.ds(0, W)] = jnp.zeros((2 * S, W), BF16)
        xs[:, pl.ds(W * (pairs + 1), W)] = jnp.zeros((2 * S, W), BF16)
        for part in range(2):
            tiles[1, pl.ds(part * 3 * W, W)] = jnp.zeros((W, W), BF16)
            tiles[pairs, pl.ds(part * 3 * W + 2 * W, W)] = jnp.zeros((W, W), BF16)

    def each_pair(body):
        def step(p, carry):
            body(p)
            return carry

        lax.fori_loop(0, pairs, step, 0, unroll=True)

    def put(p, value, slot):
        hi, lo = split(value)
        both = jnp.concatenate([hi, lo], axis=0)
        xs[:, pl.ds(pl.multiple_of(W * (p + 1), W), W)] = both
        vr[2 * p] = both[:, :BS]
        vr[2 * p + 1] = both[:, BS:]
        if slot is not None:
            keep(p, slot, hi, lo)

    def keep(p, slot, hi, lo):
        lanes = pl.ds(pl.multiple_of(W * p, W), W)
        vs[pl.ds(S * slot, S), lanes] = hi
        vs[pl.ds(4 * S + S * slot, S), lanes] = lo

    def first_field(p):
        return jnp.concatenate([v0[2 * p], v0[2 * p + 1]], axis=1)

    with jax.named_scope("load_v"):
        load_v.wait()
        each_pair(lambda p: put(p, first_field(p), 0))

    with jax.named_scope("load_l"):
        load_l.wait()
        for j in range(6):
            for s in range(H):
                hi, lo = split(lstage[j, s])
                links[j, s, pl.ds(0, BS)] = hi
                links[j, s, pl.ds(BS, BS)] = lo

    def halo_copy(step, j):
        return pltpu.make_async_remote_copy(
            src_ref=send.at[step, j],
            dst_ref=(recv0, recv1, recv2)[step].at[j ^ 1, pl.ds(1, H)],
            send_sem=halo_send.at[step],
            recv_sem=halo_recv.at[step],
            device_id=(lax.rem(me + offsets[j], n),),
            device_id_type=MESH,
        )

    def own_row(j, s):
        return jnp.minimum(rows[0, s, j], block_rows - 1)

    def multiply_link(step, j, s, mine):
        send[step, j, s] = halves(dot(jnp.concatenate([mine, mine], axis=1), links[j, s]))

    def multiply_links(step, interfaces):
        for j in interfaces:
            for s in range(H):
                multiply_link(step, j, s, vr[own_row(j, s)])

    def start_links(step, interfaces):
        for j in interfaces:
            halo_copy(step, j).start()

    def send_links(step, store):
        for j in (0, 1):
            for s in range(H):
                hi, lo = split(row_value(step - 1, own_row(j, s)))
                multiply_link(step, j, s, jnp.concatenate([hi, lo], axis=0))
        start_links(step, (0, 1))
        each_pair(store)
        multiply_links(step, (2, 3, 4, 5))
        start_links(step, (2, 3, 4, 5))

    def all_links(step):
        return pltpu.make_async_remote_copy(
            src_ref=send.at[step],
            dst_ref=(recv0, recv1, recv2)[step].at[:, pl.ds(1, H)],
            send_sem=halo_send.at[step],
            recv_sem=halo_recv.at[step],
            device_id=(lax.rem(me + 1, n),),
            device_id_type=MESH,
        )

    with jax.named_scope("links0"):
        load_r.wait()
        multiply_links(0, range(6))

    def plane_start(which, buffer, value):
        buffer[rank] = value
        for mask in plane_masks:
            pltpu.make_async_remote_copy(
                src_ref=buffer.at[rank],
                dst_ref=buffer.at[rank],
                send_sem=s1.at[which],
                recv_sem=r1.at[which],
                device_id=(me ^ mask,),
                device_id_type=MESH,
            ).start()

    def all_plane(which, buffer):
        others = buffer.at[pl.ds(0, group - 1)]
        return pltpu.make_async_remote_copy(
            src_ref=others,
            dst_ref=others,
            send_sem=s1.at[which],
            recv_sem=r1.at[which],
            device_id=(me ^ plane_masks[0],),
            device_id_type=MESH,
        )

    def plane_finish(which, buffer):
        all_plane(which, buffer).wait_recv()
        return jnp.sum(buffer[...], axis=0)

    def ring_start(which, buffer, value):
        buffer[z] = value
        for mask in ring_masks:
            pltpu.make_async_remote_copy(
                src_ref=buffer.at[z],
                dst_ref=buffer.at[z],
                send_sem=s2.at[which],
                recv_sem=r2.at[which],
                device_id=(me ^ mask,),
                device_id_type=MESH,
            ).start()

    def all_ring(which, buffer):
        others = buffer.at[pl.ds(0, zs - 1)]
        return pltpu.make_async_remote_copy(
            src_ref=others,
            dst_ref=others,
            send_sem=s2.at[which],
            recv_sem=r2.at[which],
            device_id=(me ^ ring_masks[0],),
            device_id_type=MESH,
        )

    def ring_finish(which, buffer):
        all_ring(which, buffer).wait_recv()
        return jnp.sum(buffer[...], axis=0)

    def plane_sent(which, buffer):
        all_plane(which, buffer).wait_send()

    def ring_sent(which, buffer):
        all_ring(which, buffer).wait_send()

    at = [[rows[0, s, j] for s in range(H)] for j in range(6)]
    zero_block = jnp.zeros((BS, BS), BF16)

    def split_band(c):
        load_band(c, 0).wait()
        load_band(c, 1).wait()

        @pl.loop(quarter * c, quarter * (c + 1))
        def _(p):
            for local in range(2):
                g = 2 * p + local
                for slot in range(5):
                    away = local + slot - 2
                    q = away // 2
                    hi, lo = split(stage[g, slot])
                    top = (1 - q) * W + local * BS
                    lanes = pl.ds((away % 2) * BS, BS)
                    tiles[p + q + 1, pl.ds(top, BS), lanes] = hi
                    tiles[p + q + 1, pl.ds(3 * W + top, BS), lanes] = lo
                for j in range(6):
                    found = 0
                    for s in range(H):
                        found = jnp.where(at[j][s] == g, s + 1, found)
                    inv[g * 6 + j] = found
            for part in range(2):
                tiles[p + 1, pl.ds(part * 3 * W, BS), pl.ds(BS, BS)] = zero_block
                tiles[p + 1, pl.ds(part * 3 * W + 2 * W + BS, BS), pl.ds(0, BS)] = zero_block

    def split_all():
        for c in range(4):
            split_band(c)

    steps = lax.div(me, 2 * zs)
    early = lax.rem(steps, 4) + lax.div(steps, 4) + z < 6

    @pl.when(early)
    def _():
        load_d.wait()
        split_all()

    with jax.named_scope("barrier_wait"):
        pl.semaphore_wait(barrier, 6 + group - 1 + zs - 1)
    with jax.named_scope("send0"):
        start_links(0, range(6))
    @pl.when(jnp.logical_not(early))
    def _():
        load_d.wait()

    with jax.named_scope("diagonal"):
        on_diagonal = iota((BS, BS), 0) == iota((BS, BS), 1)

        def add_diagonal(g, total):
            return total + jnp.where(on_diagonal, stage[g, 2], 0.0)

        total = lax.fori_loop(0, block_rows, add_diagonal, jnp.zeros((BS, BS), F32), unroll=4)
        mean = jnp.sum(total * (1.0 / (block_rows * BS)), axis=0, keepdims=True)
        plane_start(0, sig1, mean)

    @pl.when(jnp.logical_not(early))
    def _():
        split_all()

    def band_product():
        def body(q):
            lhs = xs[:, pl.ds(pl.multiple_of(W * q, W), 3 * W)]
            out = dot(lhs, tiles[q + 1, pl.ds(0, 3 * W)]) + dot(lhs, tiles[q + 1, pl.ds(3 * W, 3 * W)])
            out = halves(out)
            yb[2 * q], yb[2 * q + 1] = out[:, :BS], out[:, BS:]

        each_pair(body)

    def row_value(step, g):
        total = yb[g]
        for j in range(6):
            total = total + (recv0, recv1, recv2)[step][j, inv[g * 6 + j]]
        if step == 0:
            return total
        if step == 1:
            return (total * scale - w1[g]) * scale - (w1[g] * scale - v0[g])
        return total * scale - v2[g]

    def pair_value(step, p):
        return jnp.concatenate([row_value(step, 2 * p), row_value(step, 2 * p + 1)], axis=1)

    def wait_halo(step):
        all_links(step).wait_recv()

    with jax.named_scope("band0"):
        band_product()
    with jax.named_scope("halo0"):
        wait_halo(0)

    def store_w1(p):
        value = pair_value(0, p)
        w1[2 * p], w1[2 * p + 1] = value[:, :BS], value[:, BS:]
        put(p, value, None)


    with jax.named_scope("links1"):
        send_links(1, store_w1)
    with jax.named_scope("sig_ring"):
        ring_start(0, sig2, plane_finish(0, sig1))
    with jax.named_scope("band1"):
        band_product()
    with jax.named_scope("halo1"):
        wait_halo(1)
    with jax.named_scope("sig_wait"):
        sigma = jnp.sum(ring_finish(0, sig2) * (1.0 / n), axis=1, keepdims=True)
        scale = 1.0 / sigma

    def store_v2(p):
        first = jnp.concatenate([w1[2 * p], w1[2 * p + 1]], axis=1)
        keep(p, 1, *split(first * scale - first_field(p)))
        value = pair_value(1, p)
        v2[2 * p], v2[2 * p + 1] = value[:, :BS], value[:, BS:]
        put(p, value, 2)

    with jax.named_scope("links2"):
        send_links(2, store_v2)
    lane = iota((S, BS), 1)
    place = lax.div(lane, S) == lax.rem(iota((S, BS), 0), 8)
    with jax.named_scope("grams"):
        stack = jnp.concatenate([vs[pl.ds(0, 3 * S)], vs[pl.ds(4 * S, 3 * S)]], axis=0)
        grams = dot_nt(stack, stack)
        grams = grams[: 3 * S] + grams[3 * S :]
        grams = grams[:, : 3 * S] + grams[:, 3 * S :]

        def gram_of(a, b):
            return grams[S * a : S * a + S, S * b : S * b + S]

        pairs_of = ((0, 0), (0, 1), (1, 1), (1, 2), (2, 2))
        plane_start(1, gra1, jnp.stack([pack(gram_of(a, b), place) for a, b in pairs_of]))
    with jax.named_scope("band2"):
        band_product()

        def split_y(p):
            hi, lo = split(jnp.concatenate([yb[2 * p], yb[2 * p + 1]], axis=1))
            ys[:, pl.ds(pl.multiple_of(W * p, W), W)] = jnp.concatenate([hi, lo], axis=0)

        each_pair(split_y)
    with jax.named_scope("gram_y"):
        field = jnp.concatenate([vs[pl.ds(2 * S, S)], vs[pl.ds(6 * S, S)]], axis=0)
        partial = halves(dot_nt(field, ys[pl.ds(0, S)]) + dot_nt(field, ys[pl.ds(S, S)]))
        partial = partial * scale - gram_of(2, 2)
        slots = [(j, s) for j in range(6) for s in range(H)]
        mine = jnp.concatenate([vr[own_row(j, s)] for j, s in slots], axis=1)
    with jax.named_scope("halo2"):
        wait_halo(2)
    with jax.named_scope("gram_c"):
        came = [split(recv2[j, s + 1]) for j, s in slots]
        arrived = dot_nt(mine, jnp.concatenate([hi for hi, _ in came], axis=1))
        arrived = arrived + dot_nt(mine, jnp.concatenate([lo for _, lo in came], axis=1))
        last = partial + halves(arrived) * scale
        plane_start(2, grb1, pack(last, place))

    def store_v3(p):
        keep(p, 3, *split(pair_value(2, p)))

    with jax.named_scope("land2"):
        each_pair(store_v3)
    with jax.named_scope("gra_plane"):
        ring_start(1, gra2, plane_finish(1, gra1))
    with jax.named_scope("sent"):
        for step in range(3):
            all_links(step).wait_send()
        plane_sent(0, sig1)
        ring_sent(0, sig2)
        plane_sent(1, gra1)
    with jax.named_scope("grb_plane"):
        ring_start(2, grb2, plane_finish(2, grb1))
    with jax.named_scope("gra_ring"):
        moments = ring_finish(1, gra2)

    with jax.named_scope("early"):
        m = [unpack(moments[k], place) for k in range(5)]

        def across(parts):
            total = jnp.where(lane < S, parts[0], 0.0)
            for k in (1, 2):
                total = jnp.where((lane >= S * k) & (lane < S * (k + 1)), parts[k], total)
            return total

        table = jnp.concatenate(
            [
                across([m[1] + m[0], m[2] + m[1], m[3] + m[2]]),
                across([m[2] + m[1], m[3] + m[2], m[4] + m[3]]),
                across([m[3] + m[2], m[4] + m[3], m[4]]),
                across([m[0], m[1], m[2]]),
            ],
            axis=0,
        )
        table = sweep(sweep(table, 0), S)
        middle, right = table[:S], table[S:]
        known = lane < 2 * S
        gain = jnp.where(known, middle, jnp.where(lane == 2 * S + iota((S, BS), 0), -1.0, 0.0))
        base = jnp.where(known, right, 0.0)

        def of_outputs(coeffs):
            both = jnp.concatenate([coeffs * scale, -(coeffs + pltpu.roll(coeffs, S, 1))], axis=0)
            return both + pltpu.roll(both, 4 * S, 1)

        gain, base = of_outputs(gain), of_outputs(base)
        upper = [jnp.broadcast_to(middle[:, 2 * S + j : 2 * S + j + 1], (S, BS)) for j in range(S)]
        lower = [jnp.broadcast_to(right[:, 2 * S + j : 2 * S + j + 1], (S, BS)) for j in range(S)]
        from_lane = lax.rem(iota((S, BS), 0), 8) * S
        plane_sent(2, grb1)
        ring_sent(1, gra2)

    with jax.named_scope("grb_ring"):
        late = ring_finish(2, grb2)
    with jax.named_scope("late"):
        late = widen(late)
        for j in range(S):
            upper[j] = upper[j] + jnp.sum(jnp.where(lane == from_lane + j, late, 0.0), axis=1, keepdims=True)
        columns = eliminate(upper, lower)
        both = base
        for j in range(S):
            both = both - jnp.concatenate(
                [columns[j] * gain[j : j + 1], columns[j] * gain[S + j : S + j + 1]], axis=0
            )
        hi, lo = split(both)
        mixer_out[...] = jnp.concatenate([hi, lo], axis=0)
        ring_sent(2, grb2)


def mix(v0, vs, mixer, x_out, r_out, x, r, sem):
    pairs = v0.shape[0] // 2
    half = v0.shape[0] // 2
    copies = []
    for part in range(2):
        for p in range(part * pairs // 2, (part + 1) * pairs // 2):
            out = dot(mixer[...], vs[:, pl.ds(W * p, W)])
            out = out[: 2 * S] + out[2 * S :]
            for local in range(2):
                lanes = slice(BS * local, BS * local + BS)
                x[2 * p + local] = out[:S, lanes]
                r[2 * p + local] = v0[2 * p + local] + out[S:, lanes]
        at = pl.ds(half * part, half)
        copies.append(pltpu.make_async_copy(x.at[at], x_out.at[at], sem.at[part, 0]))
        copies.append(pltpu.make_async_copy(r.at[at], r_out.at[at], sem.at[part, 1]))
        copies[-2].start()
        copies[-1].start()
    for copy in copies:
        copy.wait()


def solution(mesh):
    n = mesh.devices.size
    zs = max(n // 32, 2)
    group = n // zs

    def local(right_side, band_blocks, link_blocks, link_rows):
        block_rows = right_side.shape[0]
        pairs = block_rows // 2
        field = jax.ShapeDtypeStruct(right_side.shape, F32)
        vmem = pltpu.VMEM
        dma = pltpu.SemaphoreType.DMA
        hbm = pl.BlockSpec(memory_space=pl.ANY)
        local_vmem = pl.BlockSpec(memory_space=pltpu.VMEM)
        outs = pl.pallas_call(
            functools.partial(kernel, n, zs),
            out_shape=(vmem(field.shape, F32), vmem((8 * S, W * pairs), BF16), vmem((4 * S, BS), BF16)),
            in_specs=[pl.BlockSpec(memory_space=pltpu.HBM)] * 4,
            out_specs=(local_vmem,) * 3,
            scratch_shapes=[
                pltpu.SMEM((1, H, 6), jnp.int32),
                vmem((block_rows, 5, BS, BS), F32),
                vmem((6, H, BS, BS), F32),
                vmem((pairs + 2, 6 * W, W), BF16),
                vmem((6, H, W, BS), BF16),
                vmem((2 * S, W * (pairs + 2)), BF16),
                vmem((block_rows, 2 * S, BS), BF16),
                vmem(field.shape, F32),
                vmem((2 * S, W * pairs), BF16),
                vmem(field.shape, F32),
                vmem(field.shape, F32),
                pltpu.SMEM((block_rows * 6,), jnp.int32),
                vmem((3, 6, H, S, BS), F32),
                vmem((6, H + 1, S, BS), F32),
                vmem((6, H + 1, S, BS), F32),
                vmem((6, H + 1, S, BS), F32),
                vmem((group, 1, BS), F32),
                vmem((zs, 1, BS), F32),
                vmem((group, 5, 2, BS), F32),
                vmem((zs, 5, 2, BS), F32),
                vmem((group, 2, BS), F32),
                vmem((zs, 2, BS), F32),
                dma((4,)),
                dma((4, 2)),
                dma((3,)),
                dma((3,)),
                dma((3,)),
                dma((3,)),
                dma((3,)),
                dma((3,)),
            ],
            compiler_params=pltpu.CompilerParams(
                collective_id=0, has_side_effects=True, vmem_limit_bytes=62 * 1024 * 1024
            ),
        )(
            *(
                pltpu.with_memory_space_constraint(x, pltpu.HBM)
                for x in (right_side, band_blocks, link_blocks, jnp.transpose(link_rows, (0, 2, 1)))
            )
        )
        return pl.pallas_call(
            mix,
            out_shape=(field, field),
            in_specs=[local_vmem] * 3,
            out_specs=(hbm, hbm),
            scratch_shapes=[vmem(field.shape, F32), vmem(field.shape, F32), dma((2, 2))],
        )(*(pltpu.with_memory_space_constraint(o, pltpu.VMEM) for o in outs))

    return jax.shard_map(
        local,
        mesh=mesh,
        in_specs=(P("dom", None, None), P("dom", None, None, None), P("dom", None, None, None, None), P("dom", None, None)),
        out_specs=(P("dom", None, None), P("dom", None, None)),
        check_vma=False,
    )
```

```python
import functools

import jax
import jax.numpy as jnp
from jax import lax
from jax.experimental import pallas as pl
from jax.experimental.pallas import tpu as pltpu
from jax.sharding import PartitionSpec as P

S = 16
BS = 128
W = 2 * BS
H = 4
MESH = pl.DeviceIdType.MESH
F32 = jnp.float32
BF16 = jnp.bfloat16


def dot(a, b):
    return jnp.dot(a, b, preferred_element_type=F32)


def dot_nt(a, b):
    return lax.dot_general(a, b, (((1,), (1,)), ((), ())), preferred_element_type=F32)


def split(x):
    hi = x.astype(BF16)
    return hi, (x - hi.astype(F32)).astype(BF16)


def halves(x):
    return x[:S] + x[S:]


def iota(shape, dim):
    return lax.broadcasted_iota(jnp.int32, shape, dim)


def eliminate(upper, lower):
    count = len(upper)
    for k in range(count):
        inverse = 1.0 / upper[k][k : k + 1]
        up, low = upper[k] * inverse, lower[k] * inverse
        for j in range(count):
            if j != k:
                factor = upper[j][k : k + 1]
                upper[j], lower[j] = upper[j] - up * factor, lower[j] - low * factor
        upper[k], lower[k] = up, low
    return lower


def sweep(table, first):
    lane = iota((S, BS), 1)
    rows = table.shape[0] - S

    def spread(part, k, height):
        return jnp.broadcast_to(part[:, first + k : first + k + 1], (height, BS))

    top, rest = table[:S], table[S:]
    columns = eliminate([spread(top, k, S) for k in range(S)], [spread(rest, k, rows) for k in range(S)])
    mine = (lane >= first) & (lane < first + S)
    top = jnp.where(lane == first + iota((S, BS), 0), -1.0, jnp.where(mine, 0.0, top))
    lane = iota((1, BS), 1)
    rest = jnp.where((lane >= first) & (lane < first + S), 0.0, rest)
    for k in range(S):
        rest = rest - columns[k] * top[k : k + 1]
    return rest


def pack(gram, place):
    spread = jnp.where(place, jnp.concatenate([gram] * 8, axis=1), 0.0)
    return jnp.concatenate(
        [jnp.sum(spread[:8], axis=0, keepdims=True), jnp.sum(spread[8:], axis=0, keepdims=True)], axis=0
    )


def widen(packed):
    return jnp.concatenate(
        [jnp.broadcast_to(packed[:1], (8, BS)), jnp.broadcast_to(packed[1:], (8, BS))], axis=0
    )


def unpack(packed, place):
    spread = jnp.where(place, widen(packed), 0.0)
    for shift in (64, 32, 16):
        spread = spread + pltpu.roll(spread, shift, 1)
    return spread


def kernel(
    n,
    zs,
    rhs,
    band,
    link,
    rows_in,
    v0,
    vs,
    mixer_out,
    rows,
    stage,
    lstage,
    tiles,
    links,
    xs,
    vr,
    yb,
    ys,
    w1,
    v2,
    inv,
    send,
    recv0,
    recv1,
    recv2,
    far0,
    far1,
    far2,
    farc,
    mirror1,
    mirror2,
    sig1,
    sig2,
    gra1,
    gra2,
    grb1,
    grb2,
    in_sem,
    band_sem,
    halo_send,
    halo_recv,
    s1,
    r1,
    s2,
    r2,
):
    block_rows = v0.shape[0]
    pairs = block_rows // 2
    group = n // zs
    me = lax.axis_index("dom")
    core = lax.rem(me, 2)
    given = (1 - core, core, 2, 3, 4, 5)
    facing = (
        lax.rem(me + (n - 1) + 2 * core, n),
        me ^ 1,
        lax.rem(me + n // 16, n),
        lax.rem(me + (n - n // 16), n),
        lax.rem(me + n // 4, n),
        lax.rem(me + (n - n // 4), n),
    )
    arrives_at = (0, 1, 3, 2, 5, 4)
    z = lax.rem(lax.div(me, 2), zs)
    rank = lax.div(me, 2 * zs) * 2 + lax.rem(me, 2)

    def hops(i):
        return sum((0, 1, 2, 1)[i >> at & 3] for at in (1, 3))

    plane_masks = [i // 2 * 2 * zs + i % 2 for i in sorted(range(1, group), key=hops, reverse=True)]
    ring_masks = [2 * i for i in sorted(range(1, zs), key=(0, 1, 3, 2, 7, 6, 5, 4).index if zs == 8 else None, reverse=True)]

    barrier = pltpu.get_barrier_semaphore()

    def announce(device):
        pl.semaphore_signal(barrier, inc=1, device_id=(device,), device_id_type=MESH)

    load_r = pltpu.make_async_copy(rows_in, rows, in_sem.at[0])
    load_v = pltpu.make_async_copy(rhs, v0, in_sem.at[1])
    load_l = pltpu.make_async_copy(link.at[0], lstage, in_sem.at[2])
    load_d = pltpu.make_async_copy(band.at[:, 2], stage.at[:, 2], in_sem.at[3])
    quarter = pairs // 4

    def load_band(c, side):
        at = (pl.ds(2 * quarter * c, 2 * quarter), pl.ds(3 * side, 2))
        return pltpu.make_async_copy(band.at[at], stage.at[at], band_sem.at[c, side])

    with jax.named_scope("signals"):
        for device in facing:
            announce(device)
        load_r.start()
        load_v.start()
        load_l.start()
        load_d.start()
        for c in range(4):
            load_band(c, 0).start()
            load_band(c, 1).start()
        for mask in ring_masks + plane_masks:
            announce(me ^ mask)

    with jax.named_scope("zeros"):
        for buffer in (recv0, recv1, recv2):
            buffer[:, 0] = jnp.zeros((5, S, BS), F32)
        for buffer in (far0, farc):
            buffer[0] = jnp.zeros((S, BS), F32)
        xs[:, pl.ds(0, W)] = jnp.zeros((2 * S, W), BF16)
        xs[:, pl.ds(W * (pairs + 1), W)] = jnp.zeros((2 * S, W), BF16)
        for part in range(2):
            tiles[1, pl.ds(part * 3 * W, W)] = jnp.zeros((W, W), BF16)
            tiles[pairs, pl.ds(part * 3 * W + 2 * W, W)] = jnp.zeros((W, W), BF16)

    def each_pair(body):
        def step(p, carry):
            body(p)
            return carry

        lax.fori_loop(0, pairs, step, 0, unroll=True)

    def put(p, value, slot):
        hi, lo = split(value)
        both = jnp.concatenate([hi, lo], axis=0)
        xs[:, pl.ds(pl.multiple_of(W * (p + 1), W), W)] = both
        vr[2 * p] = both[:, :BS]
        vr[2 * p + 1] = both[:, BS:]
        if slot is not None:
            keep(p, slot, hi, lo)

    def keep(p, slot, hi, lo):
        lanes = pl.ds(pl.multiple_of(W * p, W), W)
        vs[pl.ds(S * slot, S), lanes] = hi
        vs[pl.ds(4 * S + S * slot, S), lanes] = lo

    def first_field(p):
        return jnp.concatenate([v0[2 * p], v0[2 * p + 1]], axis=1)

    with jax.named_scope("load_v"):
        load_v.wait()
        each_pair(lambda p: put(p, first_field(p), 0))

    with jax.named_scope("load_l"):
        load_l.wait()
        for j in range(6):
            for s in range(H):
                hi, lo = split(lstage[given[j], s])
                links[j, s, pl.ds(0, BS)] = hi
                links[j, s, pl.ds(BS, BS)] = lo

    others = pl.ds(1, 5)
    slots = pl.ds(1, H)
    recvs, fars = (recv0, recv1, recv2), (far0, far1, far2)

    def halo_copy(step, j):
        return pltpu.make_async_remote_copy(
            src_ref=send.at[step, j],
            dst_ref=recvs[step].at[arrives_at[j] - 1, slots] if j else fars[step].at[slots],
            send_sem=halo_send.at[step],
            recv_sem=halo_recv.at[step, min(j, 1)],
            device_id=(facing[j],),
            device_id_type=MESH,
        )

    def own_row(j, s):
        return jnp.minimum(rows[0, s, given[j]], block_rows - 1)

    def times_block(j, s, mine):
        return halves(dot(jnp.concatenate([mine, mine], axis=1), links[j, s]))

    def times_transpose(s, value):
        both = jnp.concatenate(split(value), axis=0)
        return halves(dot_nt(both, links[0, s, pl.ds(0, BS)]) + dot_nt(both, links[0, s, pl.ds(BS, BS)]))

    def multiply_links(step, interfaces):
        for j in interfaces:
            for s in range(H):
                send[step, j, s] = times_block(j, s, vr[own_row(j, s)])

    def start_links(step, interfaces):
        for j in interfaces:
            halo_copy(step, j).start()

    def send_links(step, store):
        for s in range(H):
            parts = split(row_value(step - 1, own_row(0, s), False))
            send[step, 0, s] = times_block(0, s, jnp.concatenate(parts, axis=0))
        start_links(step, (0,))
        wait_far(step - 1)
        each_pair(store)
        for interfaces in ((2, 3), (4, 5, 1)):
            multiply_links(step, interfaces)
            start_links(step, interfaces)

    def wait_far(step):
        halo_copy(step, 0).wait_recv()
        if step > 0:
            for s in range(H):
                missing = mirror1[s] if step == 1 else mirror2[s] * (scale * scale)
                farc[s + 1] = fars[step][s + 1] + missing

    def wait_others(step):
        pltpu.make_async_remote_copy(
            src_ref=send.at[step, others],
            dst_ref=recvs[step].at[:, slots],
            send_sem=halo_send.at[step],
            recv_sem=halo_recv.at[step, 1],
            device_id=(facing[1],),
            device_id_type=MESH,
        ).wait_recv()

    def links_sent(step):
        pltpu.make_async_remote_copy(
            src_ref=send.at[step],
            dst_ref=send.at[step],
            send_sem=halo_send.at[step],
            recv_sem=halo_recv.at[step, 1],
            device_id=(facing[1],),
            device_id_type=MESH,
        ).wait_send()

    with jax.named_scope("links0"):
        load_r.wait()
        multiply_links(0, range(6))

    def plane_start(which, buffer, value):
        buffer[rank] = value
        for mask in plane_masks:
            pltpu.make_async_remote_copy(
                src_ref=buffer.at[rank],
                dst_ref=buffer.at[rank],
                send_sem=s1.at[which],
                recv_sem=r1.at[which],
                device_id=(me ^ mask,),
                device_id_type=MESH,
            ).start()

    def all_plane(which, buffer):
        others = buffer.at[pl.ds(0, group - 1)]
        return pltpu.make_async_remote_copy(
            src_ref=others,
            dst_ref=others,
            send_sem=s1.at[which],
            recv_sem=r1.at[which],
            device_id=(me ^ plane_masks[0],),
            device_id_type=MESH,
        )

    def plane_finish(which, buffer):
        all_plane(which, buffer).wait_recv()
        return jnp.sum(buffer[...], axis=0)

    def ring_start(which, buffer, value):
        buffer[z] = value
        for mask in ring_masks:
            pltpu.make_async_remote_copy(
                src_ref=buffer.at[z],
                dst_ref=buffer.at[z],
                send_sem=s2.at[which],
                recv_sem=r2.at[which],
                device_id=(me ^ mask,),
                device_id_type=MESH,
            ).start()

    def all_ring(which, buffer):
        others = buffer.at[pl.ds(0, zs - 1)]
        return pltpu.make_async_remote_copy(
            src_ref=others,
            dst_ref=others,
            send_sem=s2.at[which],
            recv_sem=r2.at[which],
            device_id=(me ^ ring_masks[0],),
            device_id_type=MESH,
        )

    def ring_finish(which, buffer):
        all_ring(which, buffer).wait_recv()
        return jnp.sum(buffer[...], axis=0)

    def plane_sent(which, buffer):
        all_plane(which, buffer).wait_send()

    def ring_sent(which, buffer):
        all_ring(which, buffer).wait_send()

    at = [[rows[0, s, given[j]] for s in range(H)] for j in range(6)]
    zero_block = jnp.zeros((BS, BS), BF16)

    def split_chunk(c, carry):
        load_band(c, 0).wait()
        load_band(c, 1).wait()

        @pl.loop(quarter * c, quarter * (c + 1))
        def _(p):
            for local in range(2):
                g = 2 * p + local
                for slot in range(5):
                    away = local + slot - 2
                    q = away // 2
                    hi, lo = split(stage[g, slot])
                    top = (1 - q) * W + local * BS
                    lanes = pl.ds((away % 2) * BS, BS)
                    tiles[p + q + 1, pl.ds(top, BS), lanes] = hi
                    tiles[p + q + 1, pl.ds(3 * W + top, BS), lanes] = lo
                for j in range(6):
                    found = 0
                    for s in range(H):
                        found = jnp.where(at[j][s] == g, s + 1, found)
                    inv[g * 6 + j] = found
            for part in range(2):
                tiles[p + 1, pl.ds(part * 3 * W, BS), pl.ds(BS, BS)] = zero_block
                tiles[p + 1, pl.ds(part * 3 * W + 2 * W + BS, BS), pl.ds(0, BS)] = zero_block

        return carry

    steps = lax.div(me, 2 * zs)
    away = jnp.minimum(lax.rem(steps, 4), 2) + jnp.minimum(lax.div(steps, 4), 2)
    ahead = jnp.where(away == 2, 1, 0)
    ahead = jnp.where(z == 3, 2, ahead)
    ahead = jnp.where((z < 3) | (away < 2), 4, ahead)

    @pl.when(ahead > 0)
    def _():
        load_d.wait()

    lax.fori_loop(0, ahead, split_chunk, 0)

    with jax.named_scope("barrier_wait"):
        pl.semaphore_wait(barrier, 6 + group - 1 + zs - 1)
    with jax.named_scope("send0"):
        start_links(0, range(6))
    @pl.when(ahead == 0)
    def _():
        load_d.wait()

    with jax.named_scope("diagonal"):
        on_diagonal = iota((BS, BS), 0) == iota((BS, BS), 1)

        def add_diagonal(g, total):
            return total + jnp.where(on_diagonal, stage[g, 2], 0.0)

        total = lax.fori_loop(0, block_rows, add_diagonal, jnp.zeros((BS, BS), F32), unroll=4)
        mean = jnp.sum(total * (1.0 / (block_rows * BS)), axis=0, keepdims=True)
        plane_start(0, sig1, mean)

    lax.fori_loop(ahead, 4, split_chunk, 0)

    def band_product():
        def body(q):
            lhs = xs[:, pl.ds(pl.multiple_of(W * q, W), 3 * W)]
            out = dot(lhs, tiles[q + 1, pl.ds(0, 3 * W)]) + dot(lhs, tiles[q + 1, pl.ds(3 * W, 3 * W)])
            out = halves(out)
            yb[2 * q], yb[2 * q + 1] = out[:, :BS], out[:, BS:]

        each_pair(body)

    def row_value(step, g, with_far=True):
        total = yb[g]
        for j in range(1, 6):
            total = total + recvs[step][j - 1, inv[g * 6 + j]]
        if with_far:
            total = total + (farc if step else far0)[inv[g * 6]]
        if step == 0:
            return total
        if step == 1:
            return (total * scale - w1[g]) * scale - (w1[g] * scale - v0[g])
        return total * scale - v2[g]

    def pair_value(step, p):
        return jnp.concatenate([row_value(step, 2 * p), row_value(step, 2 * p + 1)], axis=1)

    with jax.named_scope("band0"):
        band_product()
    with jax.named_scope("halo0"):
        wait_others(0)

    def store_w1(p):
        value = pair_value(0, p)
        w1[2 * p], w1[2 * p + 1] = value[:, :BS], value[:, BS:]
        put(p, value, None)


    with jax.named_scope("links1"):
        send_links(1, store_w1)
    with jax.named_scope("sig_ring"):
        ring_start(0, sig2, plane_finish(0, sig1))
    with jax.named_scope("mirror"):
        for s in range(H):
            mirror1[s] = times_transpose(s, send[0, 0, s])
            mirror2[s] = times_transpose(s, times_block(0, s, vr[own_row(0, s)]))
    with jax.named_scope("band1"):
        band_product()
    with jax.named_scope("halo1"):
        wait_others(1)
    with jax.named_scope("sig_wait"):
        sigma = jnp.sum(ring_finish(0, sig2) * (1.0 / n), axis=1, keepdims=True)
        scale = 1.0 / sigma

    def store_v2(p):
        first = jnp.concatenate([w1[2 * p], w1[2 * p + 1]], axis=1)
        keep(p, 1, *split(first * scale - first_field(p)))
        value = pair_value(1, p)
        v2[2 * p], v2[2 * p + 1] = value[:, :BS], value[:, BS:]
        put(p, value, 2)

    with jax.named_scope("links2"):
        send_links(2, store_v2)
    lane = iota((S, BS), 1)
    place = lax.div(lane, S) == lax.rem(iota((S, BS), 0), 8)
    with jax.named_scope("grams"):
        stack = jnp.concatenate([vs[pl.ds(0, 3 * S)], vs[pl.ds(4 * S, 3 * S)]], axis=0)
        grams = dot_nt(stack, stack)
        grams = grams[: 3 * S] + grams[3 * S :]
        grams = grams[:, : 3 * S] + grams[:, 3 * S :]

        def gram_of(a, b):
            return grams[S * a : S * a + S, S * b : S * b + S]

        pairs_of = ((0, 0), (0, 1), (1, 1), (1, 2), (2, 2))
        plane_start(1, gra1, jnp.stack([pack(gram_of(a, b), place) for a, b in pairs_of]))
    with jax.named_scope("band2"):
        band_product()

        def split_y(p):
            hi, lo = split(jnp.concatenate([yb[2 * p], yb[2 * p + 1]], axis=1))
            ys[:, pl.ds(pl.multiple_of(W * p, W), W)] = jnp.concatenate([hi, lo], axis=0)

        each_pair(split_y)
    with jax.named_scope("gram_y"):
        field = jnp.concatenate([vs[pl.ds(2 * S, S)], vs[pl.ds(6 * S, S)]], axis=0)
        partial = halves(dot_nt(field, ys[pl.ds(0, S)]) + dot_nt(field, ys[pl.ds(S, S)]))
        partial = partial * scale - gram_of(2, 2)
        mine = [
            jnp.concatenate([vr[own_row(j, s)] for s in range(H)], axis=1) for j in range(6)
        ]

    def gram_of_arrived(own, came):
        parts = [split(value) for value in came]
        return dot_nt(own, jnp.concatenate([hi for hi, _ in parts], axis=1)) + dot_nt(
            own, jnp.concatenate([lo for _, lo in parts], axis=1)
        )

    with jax.named_scope("halo2"):
        wait_others(2)
    with jax.named_scope("gram_o"):
        came = [recv2[j, s + 1] for j in range(5) for s in range(H)]
        partial = partial + halves(gram_of_arrived(jnp.concatenate(mine[1:], axis=1), came)) * scale
    with jax.named_scope("far2"):
        wait_far(2)
    with jax.named_scope("gram_c"):
        came = [farc[s + 1] for s in range(H)]
        last = partial + halves(gram_of_arrived(mine[0], came)) * scale
        plane_start(2, grb1, pack(last, place))

    def store_v3(p):
        keep(p, 3, *split(pair_value(2, p)))

    with jax.named_scope("land2"):
        each_pair(store_v3)
    with jax.named_scope("gra_plane"):
        ring_start(1, gra2, plane_finish(1, gra1))
    with jax.named_scope("sent"):
        for step in range(3):
            links_sent(step)
        plane_sent(0, sig1)
        ring_sent(0, sig2)
        plane_sent(1, gra1)
    with jax.named_scope("grb_plane"):
        ring_start(2, grb2, plane_finish(2, grb1))
    with jax.named_scope("gra_ring"):
        moments = ring_finish(1, gra2)

    with jax.named_scope("early"):
        m = [unpack(moments[k], place) for k in range(5)]

        def across(parts):
            total = jnp.where(lane < S, parts[0], 0.0)
            for k in (1, 2):
                total = jnp.where((lane >= S * k) & (lane < S * (k + 1)), parts[k], total)
            return total

        table = jnp.concatenate(
            [
                across([m[1] + m[0], m[2] + m[1], m[3] + m[2]]),
                across([m[2] + m[1], m[3] + m[2], m[4] + m[3]]),
                across([m[3] + m[2], m[4] + m[3], m[4]]),
                across([m[0], m[1], m[2]]),
            ],
            axis=0,
        )
        table = sweep(sweep(table, 0), S)
        middle, right = table[:S], table[S:]
        known = lane < 2 * S
        gain = jnp.where(known, middle, jnp.where(lane == 2 * S + iota((S, BS), 0), -1.0, 0.0))
        base = jnp.where(known, right, 0.0)

        def of_outputs(coeffs):
            both = jnp.concatenate([coeffs * scale, -(coeffs + pltpu.roll(coeffs, S, 1))], axis=0)
            return both + pltpu.roll(both, 4 * S, 1)

        gain, base = of_outputs(gain), of_outputs(base)
        upper = [jnp.broadcast_to(middle[:, 2 * S + j : 2 * S + j + 1], (S, BS)) for j in range(S)]
        lower = [jnp.broadcast_to(right[:, 2 * S + j : 2 * S + j + 1], (S, BS)) for j in range(S)]
        from_lane = lax.rem(iota((S, BS), 0), 8) * S
        plane_sent(2, grb1)
        ring_sent(1, gra2)

    with jax.named_scope("grb_ring"):
        late = ring_finish(2, grb2)
    with jax.named_scope("late"):
        late = widen(late)
        for j in range(S):
            upper[j] = upper[j] + jnp.sum(jnp.where(lane == from_lane + j, late, 0.0), axis=1, keepdims=True)
        columns = eliminate(upper, lower)
        both = base
        for j in range(S):
            both = both - jnp.concatenate(
                [columns[j] * gain[j : j + 1], columns[j] * gain[S + j : S + j + 1]], axis=0
            )
        hi, lo = split(both)
        mixer_out[...] = jnp.concatenate([hi, lo], axis=0)
        ring_sent(2, grb2)


def mix(v0, vs, mixer, x_out, r_out, x, r, sem):
    pairs = v0.shape[0] // 2
    half = v0.shape[0] // 2
    copies = []
    for part in range(2):
        for p in range(part * pairs // 2, (part + 1) * pairs // 2):
            out = dot(mixer[...], vs[:, pl.ds(W * p, W)])
            out = out[: 2 * S] + out[2 * S :]
            for local in range(2):
                lanes = slice(BS * local, BS * local + BS)
                x[2 * p + local] = out[:S, lanes]
                r[2 * p + local] = v0[2 * p + local] + out[S:, lanes]
        at = pl.ds(half * part, half)
        copies.append(pltpu.make_async_copy(x.at[at], x_out.at[at], sem.at[part, 0]))
        copies.append(pltpu.make_async_copy(r.at[at], r_out.at[at], sem.at[part, 1]))
        copies[-2].start()
        copies[-1].start()
    for copy in copies:
        copy.wait()


def solution(mesh):
    n = mesh.devices.size
    zs = max(n // 32, 2)
    group = n // zs

    def local(right_side, band_blocks, link_blocks, link_rows):
        block_rows = right_side.shape[0]
        pairs = block_rows // 2
        field = jax.ShapeDtypeStruct(right_side.shape, F32)
        vmem = pltpu.VMEM
        dma = pltpu.SemaphoreType.DMA
        hbm = pl.BlockSpec(memory_space=pl.ANY)
        local_vmem = pl.BlockSpec(memory_space=pltpu.VMEM)
        outs = pl.pallas_call(
            functools.partial(kernel, n, zs),
            out_shape=(vmem(field.shape, F32), vmem((8 * S, W * pairs), BF16), vmem((4 * S, BS), BF16)),
            in_specs=[pl.BlockSpec(memory_space=pltpu.HBM)] * 4,
            out_specs=(local_vmem,) * 3,
            scratch_shapes=[
                pltpu.SMEM((1, H, 6), jnp.int32),
                vmem((block_rows, 5, BS, BS), F32),
                vmem((6, H, BS, BS), F32),
                vmem((pairs + 2, 6 * W, W), BF16),
                vmem((6, H, W, BS), BF16),
                vmem((2 * S, W * (pairs + 2)), BF16),
                vmem((block_rows, 2 * S, BS), BF16),
                vmem(field.shape, F32),
                vmem((2 * S, W * pairs), BF16),
                vmem(field.shape, F32),
                vmem(field.shape, F32),
                pltpu.SMEM((block_rows * 6,), jnp.int32),
                vmem((3, 6, H, S, BS), F32),
                vmem((5, H + 1, S, BS), F32),
                vmem((5, H + 1, S, BS), F32),
                vmem((5, H + 1, S, BS), F32),
                vmem((H + 1, S, BS), F32),
                vmem((H + 1, S, BS), F32),
                vmem((H + 1, S, BS), F32),
                vmem((H + 1, S, BS), F32),
                vmem((H, S, BS), F32),
                vmem((H, S, BS), F32),
                vmem((group, 1, BS), F32),
                vmem((zs, 1, BS), F32),
                vmem((group, 5, 2, BS), F32),
                vmem((zs, 5, 2, BS), F32),
                vmem((group, 2, BS), F32),
                vmem((zs, 2, BS), F32),
                dma((4,)),
                dma((4, 2)),
                dma((3,)),
                dma((3, 2)),
                dma((3,)),
                dma((3,)),
                dma((3,)),
                dma((3,)),
            ],
            compiler_params=pltpu.CompilerParams(
                collective_id=0, has_side_effects=True, vmem_limit_bytes=62 * 1024 * 1024
            ),
        )(
            *(
                pltpu.with_memory_space_constraint(x, pltpu.HBM)
                for x in (right_side, band_blocks, link_blocks, jnp.transpose(link_rows, (0, 2, 1)))
            )
        )
        return pl.pallas_call(
            mix,
            out_shape=(field, field),
            in_specs=[local_vmem] * 3,
            out_specs=(hbm, hbm),
            scratch_shapes=[vmem(field.shape, F32), vmem(field.shape, F32), dma((2, 2))],
        )(*(pltpu.with_memory_space_constraint(o, pltpu.VMEM) for o in outs))

    return jax.shard_map(
        local,
        mesh=mesh,
        in_specs=(P("dom", None, None), P("dom", None, None, None), P("dom", None, None, None, None), P("dom", None, None)),
        out_specs=(P("dom", None, None), P("dom", None, None)),
        check_vma=False,
    )
```

```python
import functools

import jax
import jax.numpy as jnp
from jax import lax
from jax.experimental import pallas as pl
from jax.experimental.pallas import tpu as pltpu
from jax.sharding import PartitionSpec as P

S = 16
BS = 128
W = 2 * BS
H = 4
MESH = pl.DeviceIdType.MESH
F32 = jnp.float32
BF16 = jnp.bfloat16


def dot(a, b):
    return jnp.dot(a, b, preferred_element_type=F32)


def dot_nt(a, b):
    return lax.dot_general(a, b, (((1,), (1,)), ((), ())), preferred_element_type=F32)


def split(x):
    hi = x.astype(BF16)
    return hi, (x - hi.astype(F32)).astype(BF16)


def halves(x):
    return x[:S] + x[S:]


def iota(shape, dim):
    return lax.broadcasted_iota(jnp.int32, shape, dim)


def eliminate(upper, lower):
    count = len(upper)
    for k in range(count):
        inverse = 1.0 / upper[k][k : k + 1]
        up, low = upper[k] * inverse, lower[k] * inverse
        for j in range(count):
            if j != k:
                factor = upper[j][k : k + 1]
                upper[j], lower[j] = upper[j] - up * factor, lower[j] - low * factor
        upper[k], lower[k] = up, low
    return lower


def sweep(table, first):
    lane = iota((S, BS), 1)
    rows = table.shape[0] - S

    def spread(part, k, height):
        return jnp.broadcast_to(part[:, first + k : first + k + 1], (height, BS))

    top, rest = table[:S], table[S:]
    columns = eliminate([spread(top, k, S) for k in range(S)], [spread(rest, k, rows) for k in range(S)])
    mine = (lane >= first) & (lane < first + S)
    top = jnp.where(lane == first + iota((S, BS), 0), -1.0, jnp.where(mine, 0.0, top))
    lane = iota((1, BS), 1)
    rest = jnp.where((lane >= first) & (lane < first + S), 0.0, rest)
    for k in range(S):
        rest = rest - columns[k] * top[k : k + 1]
    return rest


def pack(gram, place):
    spread = jnp.where(place, jnp.concatenate([gram] * 8, axis=1), 0.0)
    return jnp.concatenate(
        [jnp.sum(spread[:8], axis=0, keepdims=True), jnp.sum(spread[8:], axis=0, keepdims=True)], axis=0
    )


def widen(packed):
    return jnp.concatenate(
        [jnp.broadcast_to(packed[:1], (8, BS)), jnp.broadcast_to(packed[1:], (8, BS))], axis=0
    )


def unpack(packed, place):
    spread = jnp.where(place, widen(packed), 0.0)
    for shift in (64, 32, 16):
        spread = spread + pltpu.roll(spread, shift, 1)
    return spread


def kernel(
    n,
    zs,
    rhs,
    band,
    link,
    rows_in,
    v0,
    vs,
    mixer_out,
    rows,
    stage,
    lstage,
    tiles,
    links,
    xs,
    vr,
    yb,
    ys,
    w1,
    v2,
    inv,
    send,
    recv0,
    recv1,
    recv2,
    far0,
    far1,
    far2,
    farc,
    mirror1,
    mirror2,
    own_mean,
    means,
    sig1,
    sig2,
    gra1,
    gra2,
    grb1,
    grb2,
    in_sem,
    band_sem,
    halo_send,
    halo_recv,
    s1,
    r1,
    s2,
    r2,
    mean_sem,
):
    block_rows = v0.shape[0]
    pairs = block_rows // 2
    group = n // zs
    me = lax.axis_index("dom")
    core = lax.rem(me, 2)
    given = (1 - core, core, 2, 3, 4, 5)
    facing = (
        lax.rem(me + (n - 1) + 2 * core, n),
        me ^ 1,
        lax.rem(me + n // 16, n),
        lax.rem(me + (n - n // 16), n),
        lax.rem(me + n // 4, n),
        lax.rem(me + (n - n // 4), n),
    )
    arrives_at = (0, 1, 3, 2, 5, 4)
    z = lax.rem(lax.div(me, 2), zs)
    rank = lax.div(me, 2 * zs) * 2 + lax.rem(me, 2)

    def hops(i):
        return sum((0, 1, 2, 1)[i >> at & 3] for at in (1, 3))

    plane_masks = [i // 2 * 2 * zs + i % 2 for i in sorted(range(1, group), key=hops, reverse=True)]
    ring_masks = [2 * i for i in sorted(range(1, zs), key=(0, 1, 3, 2, 7, 6, 5, 4).index if zs == 8 else None, reverse=True)]

    barrier = pltpu.get_barrier_semaphore()

    def announce(device):
        pl.semaphore_signal(barrier, inc=1, device_id=(device,), device_id_type=MESH)

    load_r = pltpu.make_async_copy(rows_in, rows, in_sem.at[0])
    load_v = pltpu.make_async_copy(rhs, v0, in_sem.at[1])
    load_l = pltpu.make_async_copy(link.at[0], lstage, in_sem.at[2])
    load_d = pltpu.make_async_copy(band.at[:, 2], stage.at[:, 2], in_sem.at[3])
    quarter = pairs // 4

    def load_band(c, side):
        at = (pl.ds(2 * quarter * c, 2 * quarter), pl.ds(3 * side, 2))
        return pltpu.make_async_copy(band.at[at], stage.at[at], band_sem.at[c, side])

    with jax.named_scope("signals"):
        for device in facing:
            announce(device)
        load_r.start()
        load_v.start()
        load_l.start()
        load_d.start()
        for c in range(4):
            load_band(c, 0).start()
            load_band(c, 1).start()
        for mask in ring_masks + plane_masks:
            announce(me ^ mask)

    with jax.named_scope("zeros"):
        for buffer in (recv0, recv1, recv2):
            buffer[:, 0] = jnp.zeros((5, S, BS), F32)
        for buffer in (far0, farc):
            buffer[0] = jnp.zeros((S, BS), F32)
        xs[:, pl.ds(0, W)] = jnp.zeros((2 * S, W), BF16)
        xs[:, pl.ds(W * (pairs + 1), W)] = jnp.zeros((2 * S, W), BF16)
        for part in range(2):
            tiles[1, pl.ds(part * 3 * W, W)] = jnp.zeros((W, W), BF16)
            tiles[pairs, pl.ds(part * 3 * W + 2 * W, W)] = jnp.zeros((W, W), BF16)

    def each_pair(body):
        def step(p, carry):
            body(p)
            return carry

        lax.fori_loop(0, pairs, step, 0, unroll=True)

    def put(p, value, slot):
        hi, lo = split(value)
        both = jnp.concatenate([hi, lo], axis=0)
        xs[:, pl.ds(pl.multiple_of(W * (p + 1), W), W)] = both
        vr[2 * p] = both[:, :BS]
        vr[2 * p + 1] = both[:, BS:]
        if slot is not None:
            keep(p, slot, hi, lo)

    def keep(p, slot, hi, lo):
        lanes = pl.ds(pl.multiple_of(W * p, W), W)
        vs[pl.ds(S * slot, S), lanes] = hi
        vs[pl.ds(4 * S + S * slot, S), lanes] = lo

    def first_field(p):
        return jnp.concatenate([v0[2 * p], v0[2 * p + 1]], axis=1)

    with jax.named_scope("load_v"):
        load_v.wait()
        each_pair(lambda p: put(p, first_field(p), 0))

    with jax.named_scope("load_l"):
        load_l.wait()
        for j in range(6):
            for s in range(H):
                hi, lo = split(lstage[given[j], s])
                links[j, s, pl.ds(0, BS)] = hi
                links[j, s, pl.ds(BS, BS)] = lo

    others = pl.ds(1, 5)
    slots = pl.ds(1, H)
    recvs, fars = (recv0, recv1, recv2), (far0, far1, far2)

    def halo_copy(step, j):
        return pltpu.make_async_remote_copy(
            src_ref=send.at[step, j],
            dst_ref=recvs[step].at[arrives_at[j] - 1, slots] if j else fars[step].at[slots],
            send_sem=halo_send.at[step],
            recv_sem=halo_recv.at[step, min(j, 1)],
            device_id=(facing[j],),
            device_id_type=MESH,
        )

    def own_row(j, s):
        return jnp.minimum(rows[0, s, given[j]], block_rows - 1)

    def times_block(j, s, mine):
        return halves(dot(jnp.concatenate([mine, mine], axis=1), links[j, s]))

    def times_transpose(s, value):
        both = jnp.concatenate(split(value), axis=0)
        return halves(dot_nt(both, links[0, s, pl.ds(0, BS)]) + dot_nt(both, links[0, s, pl.ds(BS, BS)]))

    def multiply_links(step, interfaces):
        for j in interfaces:
            for s in range(H):
                send[step, j, s] = times_block(j, s, vr[own_row(j, s)])

    def start_links(step, interfaces):
        for j in interfaces:
            halo_copy(step, j).start()

    def send_links(step, store):
        for s in range(H):
            parts = split(row_value(step - 1, own_row(0, s), False))
            send[step, 0, s] = times_block(0, s, jnp.concatenate(parts, axis=0))
        start_links(step, (0,))
        wait_far(step - 1)
        for j in (2, 3):
            for s in range(H):
                parts = split(row_value(step - 1, own_row(j, s)))
                send[step, j, s] = times_block(j, s, jnp.concatenate(parts, axis=0))
        start_links(step, (2, 3))
        each_pair(store)
        multiply_links(step, (4, 5, 1))
        start_links(step, (4, 5, 1))

    def wait_far(step):
        halo_copy(step, 0).wait_recv()
        if step > 0:
            for s in range(H):
                missing = mirror1[s] if step == 1 else mirror2[s] * (ratio * ratio)
                farc[s + 1] = fars[step][s + 1] + missing

    def wait_others(step):
        pltpu.make_async_remote_copy(
            src_ref=send.at[step, others],
            dst_ref=recvs[step].at[:, slots],
            send_sem=halo_send.at[step],
            recv_sem=halo_recv.at[step, 1],
            device_id=(facing[1],),
            device_id_type=MESH,
        ).wait_recv()

    def links_sent(step):
        pltpu.make_async_remote_copy(
            src_ref=send.at[step],
            dst_ref=send.at[step],
            send_sem=halo_send.at[step],
            recv_sem=halo_recv.at[step, 1],
            device_id=(facing[1],),
            device_id_type=MESH,
        ).wait_send()

    with jax.named_scope("links0"):
        load_r.wait()
        multiply_links(0, range(6))

    def mean_copy(j):
        return pltpu.make_async_remote_copy(
            src_ref=own_mean,
            dst_ref=means.at[arrives_at[j]],
            send_sem=mean_sem.at[0],
            recv_sem=mean_sem.at[1],
            device_id=(facing[j],),
            device_id_type=MESH,
        )

    def all_means():
        return pltpu.make_async_remote_copy(
            src_ref=means,
            dst_ref=means,
            send_sem=mean_sem.at[0],
            recv_sem=mean_sem.at[1],
            device_id=(facing[1],),
            device_id_type=MESH,
        )

    def plane_start(which, buffer, value):
        buffer[rank] = value
        for mask in plane_masks:
            pltpu.make_async_remote_copy(
                src_ref=buffer.at[rank],
                dst_ref=buffer.at[rank],
                send_sem=s1.at[which],
                recv_sem=r1.at[which],
                device_id=(me ^ mask,),
                device_id_type=MESH,
            ).start()

    def all_plane(which, buffer):
        others = buffer.at[pl.ds(0, group - 1)]
        return pltpu.make_async_remote_copy(
            src_ref=others,
            dst_ref=others,
            send_sem=s1.at[which],
            recv_sem=r1.at[which],
            device_id=(me ^ plane_masks[0],),
            device_id_type=MESH,
        )

    def plane_finish(which, buffer):
        all_plane(which, buffer).wait_recv()
        return jnp.sum(buffer[...], axis=0)

    def ring_start(which, buffer, value):
        buffer[z] = value
        for mask in ring_masks:
            pltpu.make_async_remote_copy(
                src_ref=buffer.at[z],
                dst_ref=buffer.at[z],
                send_sem=s2.at[which],
                recv_sem=r2.at[which],
                device_id=(me ^ mask,),
                device_id_type=MESH,
            ).start()

    def all_ring(which, buffer):
        others = buffer.at[pl.ds(0, zs - 1)]
        return pltpu.make_async_remote_copy(
            src_ref=others,
            dst_ref=others,
            send_sem=s2.at[which],
            recv_sem=r2.at[which],
            device_id=(me ^ ring_masks[0],),
            device_id_type=MESH,
        )

    def ring_finish(which, buffer):
        all_ring(which, buffer).wait_recv()
        return jnp.sum(buffer[...], axis=0)

    def plane_sent(which, buffer):
        all_plane(which, buffer).wait_send()

    def ring_sent(which, buffer):
        all_ring(which, buffer).wait_send()

    at = [[rows[0, s, given[j]] for s in range(H)] for j in range(6)]
    zero_block = jnp.zeros((BS, BS), BF16)

    def split_chunk(c, carry):
        load_band(c, 0).wait()
        load_band(c, 1).wait()

        @pl.loop(quarter * c, quarter * (c + 1))
        def _(p):
            for local in range(2):
                g = 2 * p + local
                for slot in range(5):
                    away = local + slot - 2
                    q = away // 2
                    hi, lo = split(stage[g, slot])
                    top = (1 - q) * W + local * BS
                    lanes = pl.ds((away % 2) * BS, BS)
                    tiles[p + q + 1, pl.ds(top, BS), lanes] = hi
                    tiles[p + q + 1, pl.ds(3 * W + top, BS), lanes] = lo
                for j in range(6):
                    found = 0
                    for s in range(H):
                        found = jnp.where(at[j][s] == g, s + 1, found)
                    inv[g * 6 + j] = found
            for part in range(2):
                tiles[p + 1, pl.ds(part * 3 * W, BS), pl.ds(BS, BS)] = zero_block
                tiles[p + 1, pl.ds(part * 3 * W + 2 * W + BS, BS), pl.ds(0, BS)] = zero_block

        return carry

    steps = lax.div(me, 2 * zs)
    away = jnp.minimum(lax.rem(steps, 4), 2) + jnp.minimum(lax.div(steps, 4), 2)
    ahead = jnp.where(away == 2, 1, 0)
    ahead = jnp.where(z == 3, 2, ahead)
    ahead = jnp.where((z < 3) | (away < 2), 4, ahead)

    @pl.when(ahead > 0)
    def _():
        load_d.wait()

    lax.fori_loop(0, ahead, split_chunk, 0)

    with jax.named_scope("barrier_wait"):
        pl.semaphore_wait(barrier, 6 + group - 1 + zs - 1)
    with jax.named_scope("send0"):
        start_links(0, range(6))
    @pl.when(ahead == 0)
    def _():
        load_d.wait()

    with jax.named_scope("diagonal"):
        on_diagonal = iota((BS, BS), 0) == iota((BS, BS), 1)

        def add_diagonal(g, total):
            return total + jnp.where(on_diagonal, stage[g, 2], 0.0)

        total = lax.fori_loop(0, block_rows, add_diagonal, jnp.zeros((BS, BS), F32), unroll=4)
        mean = jnp.sum(total * (1.0 / (block_rows * BS)), axis=0, keepdims=True)
        plane_start(0, sig1, mean)
        own = jnp.sum(mean, axis=1, keepdims=True)
        own_mean[...] = jnp.broadcast_to(own, (1, BS))
        for j in range(6):
            mean_copy(j).start()
        unit = 1.0 / own

    lax.fori_loop(ahead, 4, split_chunk, 0)

    def band_product():
        def body(q):
            lhs = xs[:, pl.ds(pl.multiple_of(W * q, W), 3 * W)]
            out = dot(lhs, tiles[q + 1, pl.ds(0, 3 * W)]) + dot(lhs, tiles[q + 1, pl.ds(3 * W, 3 * W)])
            out = halves(out)
            yb[2 * q], yb[2 * q + 1] = out[:, :BS], out[:, BS:]

        each_pair(body)

    def row_value(step, g, with_far=True):
        total = yb[g]
        for j in range(0 if with_far else 1, 6):
            came = recvs[step][j - 1, inv[g * 6 + j]] if j else (farc if step else far0)[inv[g * 6]]
            total = total + (came * exchange[j] if step == 1 else came)
        if step == 0:
            return total * unit
        if step == 1:
            return (total * scale - w1[g]) * ratio - (w1[g] * ratio - v0[g])
        return total * scale - v2[g]

    def pair_value(step, p):
        return jnp.concatenate([row_value(step, 2 * p), row_value(step, 2 * p + 1)], axis=1)

    with jax.named_scope("band0"):
        band_product()
    with jax.named_scope("halo0"):
        wait_others(0)

    def store_w1(p):
        value = pair_value(0, p)
        w1[2 * p], w1[2 * p + 1] = value[:, :BS], value[:, BS:]
        put(p, value, None)


    with jax.named_scope("links1"):
        send_links(1, store_w1)
    with jax.named_scope("sig_ring"):
        ring_start(0, sig2, plane_finish(0, sig1))
    with jax.named_scope("mirror"):
        all_means().wait_recv()
        exchange = [means[j] * unit for j in range(6)]
        theirs = 1.0 / means[0]
        for s in range(H):
            mirror1[s] = times_transpose(s, send[0, 0, s] * theirs)
            mirror2[s] = times_transpose(s, times_block(0, s, vr[own_row(0, s)]) * unit)
    with jax.named_scope("band1"):
        band_product()
    with jax.named_scope("halo1"):
        wait_others(1)
    with jax.named_scope("sig_wait"):
        sigma = jnp.sum(ring_finish(0, sig2) * (1.0 / n), axis=1, keepdims=True)
        scale = 1.0 / sigma
        ratio = own * scale

    def store_v2(p):
        first = jnp.concatenate([w1[2 * p], w1[2 * p + 1]], axis=1)
        keep(p, 1, *split(first * ratio - first_field(p)))
        value = pair_value(1, p)
        v2[2 * p], v2[2 * p + 1] = value[:, :BS], value[:, BS:]
        put(p, value, 2)

    with jax.named_scope("links2"):
        send_links(2, store_v2)
    lane = iota((S, BS), 1)
    place = lax.div(lane, S) == lax.rem(iota((S, BS), 0), 8)
    with jax.named_scope("grams"):
        stack = jnp.concatenate([vs[pl.ds(0, 3 * S)], vs[pl.ds(4 * S, 3 * S)]], axis=0)
        grams = dot_nt(stack, stack)
        grams = grams[: 3 * S] + grams[3 * S :]
        grams = grams[:, : 3 * S] + grams[:, 3 * S :]

        def gram_of(a, b):
            return grams[S * a : S * a + S, S * b : S * b + S]

        pairs_of = ((0, 0), (0, 1), (1, 1), (1, 2), (2, 2))
        plane_start(1, gra1, jnp.stack([pack(gram_of(a, b), place) for a, b in pairs_of]))
    with jax.named_scope("band2"):
        band_product()

        def split_y(p):
            hi, lo = split(jnp.concatenate([yb[2 * p], yb[2 * p + 1]], axis=1))
            ys[:, pl.ds(pl.multiple_of(W * p, W), W)] = jnp.concatenate([hi, lo], axis=0)

        each_pair(split_y)
    with jax.named_scope("gram_y"):
        field = jnp.concatenate([vs[pl.ds(2 * S, S)], vs[pl.ds(6 * S, S)]], axis=0)
        partial = halves(dot_nt(field, ys[pl.ds(0, S)]) + dot_nt(field, ys[pl.ds(S, S)]))
        partial = partial * scale - gram_of(2, 2)
        mine = [
            jnp.concatenate([vr[own_row(j, s)] for s in range(H)], axis=1) for j in range(6)
        ]

    def gram_of_arrived(own, came):
        parts = [split(value) for value in came]
        return dot_nt(own, jnp.concatenate([hi for hi, _ in parts], axis=1)) + dot_nt(
            own, jnp.concatenate([lo for _, lo in parts], axis=1)
        )

    with jax.named_scope("halo2"):
        wait_others(2)
    with jax.named_scope("gram_o"):
        came = [recv2[j, s + 1] for j in range(5) for s in range(H)]
        partial = partial + halves(gram_of_arrived(jnp.concatenate(mine[1:], axis=1), came)) * scale
    with jax.named_scope("far2"):
        wait_far(2)
    with jax.named_scope("gram_c"):
        came = [farc[s + 1] for s in range(H)]
        last = partial + halves(gram_of_arrived(mine[0], came)) * scale
        plane_start(2, grb1, pack(last, place))

    def store_v3(p):
        keep(p, 3, *split(pair_value(2, p)))

    with jax.named_scope("land2"):
        each_pair(store_v3)
    with jax.named_scope("gra_plane"):
        ring_start(1, gra2, plane_finish(1, gra1))
    with jax.named_scope("sent"):
        for step in range(3):
            links_sent(step)
        all_means().wait_send()
        plane_sent(0, sig1)
        ring_sent(0, sig2)
        plane_sent(1, gra1)
    with jax.named_scope("grb_plane"):
        ring_start(2, grb2, plane_finish(2, grb1))
    with jax.named_scope("gra_ring"):
        moments = ring_finish(1, gra2)

    with jax.named_scope("early"):
        m = [unpack(moments[k], place) for k in range(5)]

        def across(parts):
            total = jnp.where(lane < S, parts[0], 0.0)
            for k in (1, 2):
                total = jnp.where((lane >= S * k) & (lane < S * (k + 1)), parts[k], total)
            return total

        table = jnp.concatenate(
            [
                across([m[1] + m[0], m[2] + m[1], m[3] + m[2]]),
                across([m[2] + m[1], m[3] + m[2], m[4] + m[3]]),
                across([m[3] + m[2], m[4] + m[3], m[4]]),
                across([m[0], m[1], m[2]]),
            ],
            axis=0,
        )
        table = sweep(sweep(table, 0), S)
        middle, right = table[:S], table[S:]
        known = lane < 2 * S
        gain = jnp.where(known, middle, jnp.where(lane == 2 * S + iota((S, BS), 0), -1.0, 0.0))
        base = jnp.where(known, right, 0.0)

        def of_outputs(coeffs):
            both = jnp.concatenate([coeffs * scale, -(coeffs + pltpu.roll(coeffs, S, 1))], axis=0)
            return both + pltpu.roll(both, 4 * S, 1)

        gain, base = of_outputs(gain), of_outputs(base)
        upper = [jnp.broadcast_to(middle[:, 2 * S + j : 2 * S + j + 1], (S, BS)) for j in range(S)]
        lower = [jnp.broadcast_to(right[:, 2 * S + j : 2 * S + j + 1], (S, BS)) for j in range(S)]
        from_lane = lax.rem(iota((S, BS), 0), 8) * S
        plane_sent(2, grb1)
        ring_sent(1, gra2)

    with jax.named_scope("grb_ring"):
        late = ring_finish(2, grb2)
    with jax.named_scope("late"):
        late = widen(late)
        for j in range(S):
            upper[j] = upper[j] + jnp.sum(jnp.where(lane == from_lane + j, late, 0.0), axis=1, keepdims=True)
        columns = eliminate(upper, lower)
        both = base
        for j in range(S):
            both = both - jnp.concatenate(
                [columns[j] * gain[j : j + 1], columns[j] * gain[S + j : S + j + 1]], axis=0
            )
        hi, lo = split(both)
        mixer_out[...] = jnp.concatenate([hi, lo], axis=0)
        ring_sent(2, grb2)


def mix(v0, vs, mixer, x_out, r_out, x, r, sem):
    pairs = v0.shape[0] // 2
    half = v0.shape[0] // 2
    copies = []
    for part in range(2):
        for p in range(part * pairs // 2, (part + 1) * pairs // 2):
            out = dot(mixer[...], vs[:, pl.ds(W * p, W)])
            out = out[: 2 * S] + out[2 * S :]
            for local in range(2):
                lanes = slice(BS * local, BS * local + BS)
                x[2 * p + local] = out[:S, lanes]
                r[2 * p + local] = v0[2 * p + local] + out[S:, lanes]
        at = pl.ds(half * part, half)
        copies.append(pltpu.make_async_copy(x.at[at], x_out.at[at], sem.at[part, 0]))
        copies.append(pltpu.make_async_copy(r.at[at], r_out.at[at], sem.at[part, 1]))
        copies[-2].start()
        copies[-1].start()
    for copy in copies:
        copy.wait()


def solution(mesh):
    n = mesh.devices.size
    zs = max(n // 32, 2)
    group = n // zs

    def local(right_side, band_blocks, link_blocks, link_rows):
        block_rows = right_side.shape[0]
        pairs = block_rows // 2
        field = jax.ShapeDtypeStruct(right_side.shape, F32)
        vmem = pltpu.VMEM
        dma = pltpu.SemaphoreType.DMA
        hbm = pl.BlockSpec(memory_space=pl.ANY)
        local_vmem = pl.BlockSpec(memory_space=pltpu.VMEM)
        outs = pl.pallas_call(
            functools.partial(kernel, n, zs),
            out_shape=(vmem(field.shape, F32), vmem((8 * S, W * pairs), BF16), vmem((4 * S, BS), BF16)),
            in_specs=[pl.BlockSpec(memory_space=pltpu.HBM)] * 4,
            out_specs=(local_vmem,) * 3,
            scratch_shapes=[
                pltpu.SMEM((1, H, 6), jnp.int32),
                vmem((block_rows, 5, BS, BS), F32),
                vmem((6, H, BS, BS), F32),
                vmem((pairs + 2, 6 * W, W), BF16),
                vmem((6, H, W, BS), BF16),
                vmem((2 * S, W * (pairs + 2)), BF16),
                vmem((block_rows, 2 * S, BS), BF16),
                vmem(field.shape, F32),
                vmem((2 * S, W * pairs), BF16),
                vmem(field.shape, F32),
                vmem(field.shape, F32),
                pltpu.SMEM((block_rows * 6,), jnp.int32),
                vmem((3, 6, H, S, BS), F32),
                vmem((5, H + 1, S, BS), F32),
                vmem((5, H + 1, S, BS), F32),
                vmem((5, H + 1, S, BS), F32),
                vmem((H + 1, S, BS), F32),
                vmem((H + 1, S, BS), F32),
                vmem((H + 1, S, BS), F32),
                vmem((H + 1, S, BS), F32),
                vmem((H, S, BS), F32),
                vmem((H, S, BS), F32),
                vmem((1, BS), F32),
                vmem((6, 1, BS), F32),
                vmem((group, 1, BS), F32),
                vmem((zs, 1, BS), F32),
                vmem((group, 5, 2, BS), F32),
                vmem((zs, 5, 2, BS), F32),
                vmem((group, 2, BS), F32),
                vmem((zs, 2, BS), F32),
                dma((4,)),
                dma((4, 2)),
                dma((3,)),
                dma((3, 2)),
                dma((3,)),
                dma((3,)),
                dma((3,)),
                dma((3,)),
                dma((2,)),
            ],
            compiler_params=pltpu.CompilerParams(
                collective_id=0, has_side_effects=True, vmem_limit_bytes=62 * 1024 * 1024
            ),
        )(
            *(
                pltpu.with_memory_space_constraint(x, pltpu.HBM)
                for x in (right_side, band_blocks, link_blocks, jnp.transpose(link_rows, (0, 2, 1)))
            )
        )
        return pl.pallas_call(
            mix,
            out_shape=(field, field),
            in_specs=[local_vmem] * 3,
            out_specs=(hbm, hbm),
            scratch_shapes=[vmem(field.shape, F32), vmem(field.shape, F32), dma((2, 2))],
        )(*(pltpu.with_memory_space_constraint(o, pltpu.VMEM) for o in outs))

    return jax.shard_map(
        local,
        mesh=mesh,
        in_specs=(P("dom", None, None), P("dom", None, None, None), P("dom", None, None, None, None), P("dom", None, None)),
        out_specs=(P("dom", None, None), P("dom", None, None)),
        check_vma=False,
    )
```

```python
import functools

import jax
import jax.numpy as jnp
from jax import lax
from jax.experimental import pallas as pl
from jax.experimental.pallas import tpu as pltpu
from jax.sharding import PartitionSpec as P

S = 16
BS = 128
W = 2 * BS
H = 4
MESH = pl.DeviceIdType.MESH
F32 = jnp.float32
BF16 = jnp.bfloat16


def dot(a, b):
    return jnp.dot(a, b, preferred_element_type=F32)


def dot_nt(a, b):
    return lax.dot_general(a, b, (((1,), (1,)), ((), ())), preferred_element_type=F32)


def split(x):
    hi = x.astype(BF16)
    return hi, (x - hi.astype(F32)).astype(BF16)


def halves(x):
    return x[:S] + x[S:]


def iota(shape, dim):
    return lax.broadcasted_iota(jnp.int32, shape, dim)


def eliminate(upper, lower):
    count = len(upper)
    for k in range(count):
        inverse = 1.0 / upper[k][k : k + 1]
        up, low = upper[k] * inverse, lower[k] * inverse
        for j in range(count):
            if j != k:
                factor = upper[j][k : k + 1]
                upper[j], lower[j] = upper[j] - up * factor, lower[j] - low * factor
        upper[k], lower[k] = up, low
    return lower


def sweep(table, first):
    lane = iota((S, BS), 1)
    rows = table.shape[0] - S

    def spread(part, k, height):
        return jnp.broadcast_to(part[:, first + k : first + k + 1], (height, BS))

    top, rest = table[:S], table[S:]
    columns = eliminate([spread(top, k, S) for k in range(S)], [spread(rest, k, rows) for k in range(S)])
    mine = (lane >= first) & (lane < first + S)
    top = jnp.where(lane == first + iota((S, BS), 0), -1.0, jnp.where(mine, 0.0, top))
    lane = iota((1, BS), 1)
    rest = jnp.where((lane >= first) & (lane < first + S), 0.0, rest)
    for k in range(S):
        rest = rest - columns[k] * top[k : k + 1]
    return rest


def pack(gram, place):
    spread = jnp.where(place, jnp.concatenate([gram] * 8, axis=1), 0.0)
    return jnp.concatenate(
        [jnp.sum(spread[:8], axis=0, keepdims=True), jnp.sum(spread[8:], axis=0, keepdims=True)], axis=0
    )


def widen(packed):
    return jnp.concatenate(
        [jnp.broadcast_to(packed[:1], (8, BS)), jnp.broadcast_to(packed[1:], (8, BS))], axis=0
    )


def unpack(packed, place):
    spread = jnp.where(place, widen(packed), 0.0)
    for shift in (64, 32, 16):
        spread = spread + pltpu.roll(spread, shift, 1)
    return spread


def kernel(
    n,
    zs,
    rhs,
    band,
    link,
    rows_in,
    v0,
    vs,
    mixer_out,
    rows,
    stage,
    lstage,
    tiles,
    links,
    xs,
    vr,
    yb,
    ys,
    w1,
    v2,
    inv,
    send,
    recv0,
    recv1,
    recv2,
    far0,
    far1,
    far2,
    farc,
    mirror1,
    mirror2,
    own_mean,
    means,
    sig1,
    sig2,
    gra1,
    gra2,
    grb1,
    grb2,
    in_sem,
    band_sem,
    halo_send,
    halo_recv,
    s1,
    r1,
    s2,
    r2,
    mean_sem,
):
    block_rows = v0.shape[0]
    pairs = block_rows // 2
    group = n // zs
    me = lax.axis_index("dom")
    core = lax.rem(me, 2)
    given = (1 - core, core, 4, 5, 2, 3)
    facing = (
        lax.rem(me + (n - 1) + 2 * core, n),
        me ^ 1,
        lax.rem(me + n // 4, n),
        lax.rem(me + (n - n // 4), n),
        lax.rem(me + n // 16, n),
        lax.rem(me + (n - n // 16), n),
    )
    arrives_at = (0, 1, 3, 2, 5, 4)
    z = lax.rem(lax.div(me, 2), zs)
    rank = lax.div(me, 2 * zs) * 2 + lax.rem(me, 2)

    def hops(i):
        return sum((0, 1, 2, 1)[i >> at & 3] for at in (1, 3))

    plane_masks = [i // 2 * 2 * zs + i % 2 for i in sorted(range(1, group), key=hops, reverse=True)]
    ring_masks = [2 * i for i in sorted(range(1, zs), key=(0, 1, 3, 2, 7, 6, 5, 4).index if zs == 8 else None, reverse=True)]

    barrier = pltpu.get_barrier_semaphore()

    def announce(device):
        pl.semaphore_signal(barrier, inc=1, device_id=(device,), device_id_type=MESH)

    load_r = pltpu.make_async_copy(rows_in, rows, in_sem.at[0])
    load_v = pltpu.make_async_copy(rhs, v0, in_sem.at[1])
    load_l = pltpu.make_async_copy(link.at[0], lstage, in_sem.at[2])
    load_d = pltpu.make_async_copy(band.at[:, 2], stage.at[:, 2], in_sem.at[3])
    quarter = pairs // 4

    def load_band(c, side):
        at = (pl.ds(2 * quarter * c, 2 * quarter), pl.ds(3 * side, 2))
        return pltpu.make_async_copy(band.at[at], stage.at[at], band_sem.at[c, side])

    with jax.named_scope("signals"):
        for device in facing:
            announce(device)
        load_r.start()
        load_v.start()
        load_l.start()
        load_d.start()
        for c in range(4):
            load_band(c, 0).start()
            load_band(c, 1).start()
        for mask in ring_masks + plane_masks:
            announce(me ^ mask)

    with jax.named_scope("zeros"):
        for buffer in (recv0, recv1, recv2):
            buffer[:, 0] = jnp.zeros((5, S, BS), F32)
        for buffer in (far0, farc):
            buffer[0] = jnp.zeros((S, BS), F32)
        xs[:, pl.ds(0, W)] = jnp.zeros((2 * S, W), BF16)
        xs[:, pl.ds(W * (pairs + 1), W)] = jnp.zeros((2 * S, W), BF16)
        for part in range(2):
            tiles[1, pl.ds(part * 3 * W, W)] = jnp.zeros((W, W), BF16)
            tiles[pairs, pl.ds(part * 3 * W + 2 * W, W)] = jnp.zeros((W, W), BF16)

    def each_pair(body):
        def step(p, carry):
            body(p)
            return carry

        lax.fori_loop(0, pairs, step, 0, unroll=True)

    def put(p, value, slot):
        hi, lo = split(value)
        both = jnp.concatenate([hi, lo], axis=0)
        xs[:, pl.ds(pl.multiple_of(W * (p + 1), W), W)] = both
        vr[2 * p] = both[:, :BS]
        vr[2 * p + 1] = both[:, BS:]
        if slot is not None:
            keep(p, slot, hi, lo)

    def keep(p, slot, hi, lo):
        lanes = pl.ds(pl.multiple_of(W * p, W), W)
        vs[pl.ds(S * slot, S), lanes] = hi
        vs[pl.ds(4 * S + S * slot, S), lanes] = lo

    def first_field(p):
        return jnp.concatenate([v0[2 * p], v0[2 * p + 1]], axis=1)

    with jax.named_scope("load_v"):
        load_v.wait()
        each_pair(lambda p: put(p, first_field(p), 0))

    with jax.named_scope("load_l"):
        load_l.wait()
        for j in range(6):
            for s in range(H):
                hi, lo = split(lstage[given[j], s])
                links[j, s, pl.ds(0, BS)] = hi
                links[j, s, pl.ds(BS, BS)] = lo

    slots = pl.ds(1, H)
    recvs, fars = (recv0, recv1, recv2), (far0, far1, far2)

    def halo_copy(step, j):
        return pltpu.make_async_remote_copy(
            src_ref=send.at[step, j],
            dst_ref=recvs[step].at[arrives_at[j] - 1, slots] if j else fars[step].at[slots],
            send_sem=halo_send.at[step],
            recv_sem=halo_recv.at[step, (0, 1, 1, 1, 2, 2)[j]],
            device_id=(facing[j],),
            device_id_type=MESH,
        )

    def own_row(j, s):
        return jnp.minimum(rows[0, s, given[j]], block_rows - 1)

    def times_block(j, s, mine):
        return halves(dot(jnp.concatenate([mine, mine], axis=1), links[j, s]))

    def times_transpose(s, value):
        both = jnp.concatenate(split(value), axis=0)
        return halves(dot_nt(both, links[0, s, pl.ds(0, BS)]) + dot_nt(both, links[0, s, pl.ds(BS, BS)]))

    def multiply_links(step, interfaces):
        for j in interfaces:
            for s in range(H):
                send[step, j, s] = times_block(j, s, vr[own_row(j, s)])

    def start_links(step, interfaces):
        for j in interfaces:
            halo_copy(step, j).start()

    def send_links(step, store):
        for s in range(H):
            parts = split(row_value(step - 1, own_row(0, s), False))
            send[step, 0, s] = times_block(0, s, jnp.concatenate(parts, axis=0))
        start_links(step, (0,))
        wait_far(step - 1)
        for j in (4, 5):
            for s in range(H):
                parts = split(row_value(step - 1, own_row(j, s)))
                send[step, j, s] = times_block(j, s, jnp.concatenate(parts, axis=0))
        start_links(step, (4, 5))
        each_pair(store)
        multiply_links(step, (2, 3, 1))
        start_links(step, (2, 3, 1))

    def wait_far(step):
        halo_copy(step, 0).wait_recv()
        if step > 0:
            for s in range(H):
                missing = mirror1[s] if step == 1 else mirror2[s] * (ratio * ratio)
                farc[s + 1] = fars[step][s + 1] + missing

    def wait_group(step, which):
        group_of = pl.ds(0, 3) if which == 1 else pl.ds(3, 2)
        came = recvs[step].at[group_of, slots]
        pltpu.make_async_remote_copy(
            src_ref=came,
            dst_ref=came,
            send_sem=halo_send.at[step],
            recv_sem=halo_recv.at[step, which],
            device_id=(facing[1],),
            device_id_type=MESH,
        ).wait_recv()

    def wait_others(step):
        wait_group(step, 1)
        wait_group(step, 2)

    def links_sent(step):
        pltpu.make_async_remote_copy(
            src_ref=send.at[step],
            dst_ref=send.at[step],
            send_sem=halo_send.at[step],
            recv_sem=halo_recv.at[step, 1],
            device_id=(facing[1],),
            device_id_type=MESH,
        ).wait_send()

    with jax.named_scope("links0"):
        load_r.wait()
        multiply_links(0, range(6))

    def mean_copy(j):
        return pltpu.make_async_remote_copy(
            src_ref=own_mean,
            dst_ref=means.at[arrives_at[j]],
            send_sem=mean_sem.at[0],
            recv_sem=mean_sem.at[1],
            device_id=(facing[j],),
            device_id_type=MESH,
        )

    def all_means():
        return pltpu.make_async_remote_copy(
            src_ref=means,
            dst_ref=means,
            send_sem=mean_sem.at[0],
            recv_sem=mean_sem.at[1],
            device_id=(facing[1],),
            device_id_type=MESH,
        )

    def plane_start(which, buffer, value):
        buffer[rank] = value
        for mask in plane_masks:
            pltpu.make_async_remote_copy(
                src_ref=buffer.at[rank],
                dst_ref=buffer.at[rank],
                send_sem=s1.at[which],
                recv_sem=r1.at[which],
                device_id=(me ^ mask,),
                device_id_type=MESH,
            ).start()

    def all_plane(which, buffer):
        others = buffer.at[pl.ds(0, group - 1)]
        return pltpu.make_async_remote_copy(
            src_ref=others,
            dst_ref=others,
            send_sem=s1.at[which],
            recv_sem=r1.at[which],
            device_id=(me ^ plane_masks[0],),
            device_id_type=MESH,
        )

    def plane_finish(which, buffer):
        all_plane(which, buffer).wait_recv()
        return jnp.sum(buffer[...], axis=0)

    def ring_start(which, buffer, value):
        buffer[z] = value
        for mask in ring_masks:
            pltpu.make_async_remote_copy(
                src_ref=buffer.at[z],
                dst_ref=buffer.at[z],
                send_sem=s2.at[which],
                recv_sem=r2.at[which],
                device_id=(me ^ mask,),
                device_id_type=MESH,
            ).start()

    def all_ring(which, buffer):
        others = buffer.at[pl.ds(0, zs - 1)]
        return pltpu.make_async_remote_copy(
            src_ref=others,
            dst_ref=others,
            send_sem=s2.at[which],
            recv_sem=r2.at[which],
            device_id=(me ^ ring_masks[0],),
            device_id_type=MESH,
        )

    def ring_finish(which, buffer):
        all_ring(which, buffer).wait_recv()
        return jnp.sum(buffer[...], axis=0)

    def plane_sent(which, buffer):
        all_plane(which, buffer).wait_send()

    def ring_sent(which, buffer):
        all_ring(which, buffer).wait_send()

    at = [[rows[0, s, given[j]] for s in range(H)] for j in range(6)]
    zero_block = jnp.zeros((BS, BS), BF16)

    def split_chunk(c, carry):
        load_band(c, 0).wait()
        load_band(c, 1).wait()

        @pl.loop(quarter * c, quarter * (c + 1))
        def _(p):
            for local in range(2):
                g = 2 * p + local
                for slot in range(5):
                    away = local + slot - 2
                    q = away // 2
                    hi, lo = split(stage[g, slot])
                    top = (1 - q) * W + local * BS
                    lanes = pl.ds((away % 2) * BS, BS)
                    tiles[p + q + 1, pl.ds(top, BS), lanes] = hi
                    tiles[p + q + 1, pl.ds(3 * W + top, BS), lanes] = lo
                for j in range(6):
                    found = 0
                    for s in range(H):
                        found = jnp.where(at[j][s] == g, s + 1, found)
                    inv[g * 6 + j] = found
            for part in range(2):
                tiles[p + 1, pl.ds(part * 3 * W, BS), pl.ds(BS, BS)] = zero_block
                tiles[p + 1, pl.ds(part * 3 * W + 2 * W + BS, BS), pl.ds(0, BS)] = zero_block

        return carry

    steps = lax.div(me, 2 * zs)
    away = jnp.minimum(lax.rem(steps, 4), 2) + jnp.minimum(lax.div(steps, 4), 2)
    ahead = jnp.where(away == 2, 1, 0)
    ahead = jnp.where(z == 3, 2, ahead)
    ahead = jnp.where((z < 3) | (away < 2), 4, ahead)

    @pl.when(ahead > 0)
    def _():
        load_d.wait()

    lax.fori_loop(0, ahead, split_chunk, 0)

    with jax.named_scope("barrier_wait"):
        pl.semaphore_wait(barrier, 6 + group - 1 + zs - 1)
    with jax.named_scope("send0"):
        start_links(0, range(6))
    @pl.when(ahead == 0)
    def _():
        load_d.wait()

    with jax.named_scope("diagonal"):
        on_diagonal = iota((BS, BS), 0) == iota((BS, BS), 1)

        def add_diagonal(g, total):
            return total + jnp.where(on_diagonal, stage[g, 2], 0.0)

        total = lax.fori_loop(0, block_rows, add_diagonal, jnp.zeros((BS, BS), F32), unroll=4)
        mean = jnp.sum(total * (1.0 / (block_rows * BS)), axis=0, keepdims=True)
        plane_start(0, sig1, mean)
        own = jnp.sum(mean, axis=1, keepdims=True)
        own_mean[...] = jnp.broadcast_to(own, (1, BS))
        for j in range(6):
            mean_copy(j).start()
        unit = 1.0 / own

    lax.fori_loop(ahead, 4, split_chunk, 0)

    def band_product():
        def body(q):
            lhs = xs[:, pl.ds(pl.multiple_of(W * q, W), 3 * W)]
            out = dot(lhs, tiles[q + 1, pl.ds(0, 3 * W)]) + dot(lhs, tiles[q + 1, pl.ds(3 * W, 3 * W)])
            out = halves(out)
            yb[2 * q], yb[2 * q + 1] = out[:, :BS], out[:, BS:]

        each_pair(body)

    def row_value(step, g, with_far=True):
        total = yb[g]
        for j in range(0 if with_far else 1, 6):
            came = recvs[step][j - 1, inv[g * 6 + j]] if j else (farc if step else far0)[inv[g * 6]]
            total = total + (came * exchange[j] if step == 1 else came)
        if step == 0:
            return total * unit
        if step == 1:
            return (total * scale - w1[g]) * ratio - (w1[g] * ratio - v0[g])
        return total * scale - v2[g]

    def pair_value(step, p):
        return jnp.concatenate([row_value(step, 2 * p), row_value(step, 2 * p + 1)], axis=1)

    with jax.named_scope("band0"):
        band_product()
    with jax.named_scope("halo0"):
        wait_others(0)

    def store_w1(p):
        value = pair_value(0, p)
        w1[2 * p], w1[2 * p + 1] = value[:, :BS], value[:, BS:]
        put(p, value, None)


    with jax.named_scope("links1"):
        send_links(1, store_w1)
    with jax.named_scope("sig_ring"):
        ring_start(0, sig2, plane_finish(0, sig1))
    with jax.named_scope("mirror"):
        all_means().wait_recv()
        exchange = [means[j] * unit for j in range(6)]
        theirs = 1.0 / means[0]
        for s in range(H):
            mirror1[s] = times_transpose(s, send[0, 0, s] * theirs)
            mirror2[s] = times_transpose(s, times_block(0, s, vr[own_row(0, s)]) * unit)
    with jax.named_scope("band1"):
        band_product()
    with jax.named_scope("halo1"):
        wait_others(1)
    with jax.named_scope("sig_wait"):
        sigma = jnp.sum(ring_finish(0, sig2) * (1.0 / n), axis=1, keepdims=True)
        scale = 1.0 / sigma
        ratio = own * scale

    def store_v2(p):
        first = jnp.concatenate([w1[2 * p], w1[2 * p + 1]], axis=1)
        keep(p, 1, *split(first * ratio - first_field(p)))
        value = pair_value(1, p)
        v2[2 * p], v2[2 * p + 1] = value[:, :BS], value[:, BS:]
        put(p, value, 2)

    with jax.named_scope("links2"):
        send_links(2, store_v2)
    lane = iota((S, BS), 1)
    place = lax.div(lane, S) == lax.rem(iota((S, BS), 0), 8)
    with jax.named_scope("grams"):
        stack = jnp.concatenate([vs[pl.ds(0, 3 * S)], vs[pl.ds(4 * S, 3 * S)]], axis=0)
        grams = dot_nt(stack, stack)
        grams = grams[: 3 * S] + grams[3 * S :]
        grams = grams[:, : 3 * S] + grams[:, 3 * S :]

        def gram_of(a, b):
            return grams[S * a : S * a + S, S * b : S * b + S]

        pairs_of = ((0, 0), (0, 1), (1, 1), (1, 2), (2, 2))
        plane_start(1, gra1, jnp.stack([pack(gram_of(a, b), place) for a, b in pairs_of]))
    with jax.named_scope("band2"):
        band_product()

        def split_y(p):
            hi, lo = split(jnp.concatenate([yb[2 * p], yb[2 * p + 1]], axis=1))
            ys[:, pl.ds(pl.multiple_of(W * p, W), W)] = jnp.concatenate([hi, lo], axis=0)

        each_pair(split_y)
    with jax.named_scope("gram_y"):
        field = jnp.concatenate([vs[pl.ds(2 * S, S)], vs[pl.ds(6 * S, S)]], axis=0)
        partial = halves(dot_nt(field, ys[pl.ds(0, S)]) + dot_nt(field, ys[pl.ds(S, S)]))
        partial = partial * scale - gram_of(2, 2)
        mine = [
            jnp.concatenate([vr[own_row(j, s)] for s in range(H)], axis=1) for j in range(6)
        ]

    def gram_of_arrived(own, came):
        parts = [split(value) for value in came]
        return dot_nt(own, jnp.concatenate([hi for hi, _ in parts], axis=1)) + dot_nt(
            own, jnp.concatenate([lo for _, lo in parts], axis=1)
        )

    with jax.named_scope("halo2"):
        wait_group(2, 1)
    with jax.named_scope("gram_o"):
        came = [recv2[j, s + 1] for j in range(3) for s in range(H)]
        partial = partial + halves(gram_of_arrived(jnp.concatenate(mine[1:4], axis=1), came)) * scale
    with jax.named_scope("far2"):
        wait_group(2, 2)
        wait_far(2)
    with jax.named_scope("gram_c"):
        came = [recv2[j, s + 1] for j in (3, 4) for s in range(H)] + [farc[s + 1] for s in range(H)]
        last = partial + halves(gram_of_arrived(jnp.concatenate(mine[4:] + mine[:1], axis=1), came)) * scale
        plane_start(2, grb1, pack(last, place))

    def store_v3(p):
        keep(p, 3, *split(pair_value(2, p)))

    with jax.named_scope("land2"):
        each_pair(store_v3)
    with jax.named_scope("gra_plane"):
        ring_start(1, gra2, plane_finish(1, gra1))
    with jax.named_scope("sent"):
        for step in range(3):
            links_sent(step)
        all_means().wait_send()
        plane_sent(0, sig1)
        ring_sent(0, sig2)
        plane_sent(1, gra1)
    with jax.named_scope("grb_plane"):
        ring_start(2, grb2, plane_finish(2, grb1))
    with jax.named_scope("gra_ring"):
        moments = ring_finish(1, gra2)

    with jax.named_scope("early"):
        m = [unpack(moments[k], place) for k in range(5)]

        def across(parts):
            total = jnp.where(lane < S, parts[0], 0.0)
            for k in (1, 2):
                total = jnp.where((lane >= S * k) & (lane < S * (k + 1)), parts[k], total)
            return total

        table = jnp.concatenate(
            [
                across([m[1] + m[0], m[2] + m[1], m[3] + m[2]]),
                across([m[2] + m[1], m[3] + m[2], m[4] + m[3]]),
                across([m[3] + m[2], m[4] + m[3], m[4]]),
                across([m[0], m[1], m[2]]),
            ],
            axis=0,
        )
        table = sweep(sweep(table, 0), S)
        middle, right = table[:S], table[S:]
        known = lane < 2 * S
        gain = jnp.where(known, middle, jnp.where(lane == 2 * S + iota((S, BS), 0), -1.0, 0.0))
        base = jnp.where(known, right, 0.0)

        def of_outputs(coeffs):
            both = jnp.concatenate([coeffs * scale, -(coeffs + pltpu.roll(coeffs, S, 1))], axis=0)
            return both + pltpu.roll(both, 4 * S, 1)

        gain, base = of_outputs(gain), of_outputs(base)
        upper = [jnp.broadcast_to(middle[:, 2 * S + j : 2 * S + j + 1], (S, BS)) for j in range(S)]
        lower = [jnp.broadcast_to(right[:, 2 * S + j : 2 * S + j + 1], (S, BS)) for j in range(S)]
        from_lane = lax.rem(iota((S, BS), 0), 8) * S
        plane_sent(2, grb1)
        ring_sent(1, gra2)

    with jax.named_scope("grb_ring"):
        late = ring_finish(2, grb2)
    with jax.named_scope("late"):
        late = widen(late)
        for j in range(S):
            upper[j] = upper[j] + jnp.sum(jnp.where(lane == from_lane + j, late, 0.0), axis=1, keepdims=True)
        columns = eliminate(upper, lower)
        both = base
        for j in range(S):
            both = both - jnp.concatenate(
                [columns[j] * gain[j : j + 1], columns[j] * gain[S + j : S + j + 1]], axis=0
            )
        hi, lo = split(both)
        mixer_out[...] = jnp.concatenate([hi, lo], axis=0)
        ring_sent(2, grb2)


def mix(v0, vs, mixer, x_out, r_out, x, r, sem):
    pairs = v0.shape[0] // 2
    half = v0.shape[0] // 2
    copies = []
    for part in range(2):
        for p in range(part * pairs // 2, (part + 1) * pairs // 2):
            out = dot(mixer[...], vs[:, pl.ds(W * p, W)])
            out = out[: 2 * S] + out[2 * S :]
            for local in range(2):
                lanes = slice(BS * local, BS * local + BS)
                x[2 * p + local] = out[:S, lanes]
                r[2 * p + local] = v0[2 * p + local] + out[S:, lanes]
        at = pl.ds(half * part, half)
        copies.append(pltpu.make_async_copy(x.at[at], x_out.at[at], sem.at[part, 0]))
        copies.append(pltpu.make_async_copy(r.at[at], r_out.at[at], sem.at[part, 1]))
        copies[-2].start()
        copies[-1].start()
    for copy in copies:
        copy.wait()


def solution(mesh):
    n = mesh.devices.size
    zs = max(n // 32, 2)
    group = n // zs

    def local(right_side, band_blocks, link_blocks, link_rows):
        block_rows = right_side.shape[0]
        pairs = block_rows // 2
        field = jax.ShapeDtypeStruct(right_side.shape, F32)
        vmem = pltpu.VMEM
        dma = pltpu.SemaphoreType.DMA
        hbm = pl.BlockSpec(memory_space=pl.ANY)
        local_vmem = pl.BlockSpec(memory_space=pltpu.VMEM)
        outs = pl.pallas_call(
            functools.partial(kernel, n, zs),
            out_shape=(vmem(field.shape, F32), vmem((8 * S, W * pairs), BF16), vmem((4 * S, BS), BF16)),
            in_specs=[pl.BlockSpec(memory_space=pltpu.HBM)] * 4,
            out_specs=(local_vmem,) * 3,
            scratch_shapes=[
                pltpu.SMEM((1, H, 6), jnp.int32),
                vmem((block_rows, 5, BS, BS), F32),
                vmem((6, H, BS, BS), F32),
                vmem((pairs + 2, 6 * W, W), BF16),
                vmem((6, H, W, BS), BF16),
                vmem((2 * S, W * (pairs + 2)), BF16),
                vmem((block_rows, 2 * S, BS), BF16),
                vmem(field.shape, F32),
                vmem((2 * S, W * pairs), BF16),
                vmem(field.shape, F32),
                vmem(field.shape, F32),
                pltpu.SMEM((block_rows * 6,), jnp.int32),
                vmem((3, 6, H, S, BS), F32),
                vmem((5, H + 1, S, BS), F32),
                vmem((5, H + 1, S, BS), F32),
                vmem((5, H + 1, S, BS), F32),
                vmem((H + 1, S, BS), F32),
                vmem((H + 1, S, BS), F32),
                vmem((H + 1, S, BS), F32),
                vmem((H + 1, S, BS), F32),
                vmem((H, S, BS), F32),
                vmem((H, S, BS), F32),
                vmem((1, BS), F32),
                vmem((6, 1, BS), F32),
                vmem((group, 1, BS), F32),
                vmem((zs, 1, BS), F32),
                vmem((group, 5, 2, BS), F32),
                vmem((zs, 5, 2, BS), F32),
                vmem((group, 2, BS), F32),
                vmem((zs, 2, BS), F32),
                dma((4,)),
                dma((4, 2)),
                dma((3,)),
                dma((3, 3)),
                dma((3,)),
                dma((3,)),
                dma((3,)),
                dma((3,)),
                dma((2,)),
            ],
            compiler_params=pltpu.CompilerParams(
                collective_id=0, has_side_effects=True, vmem_limit_bytes=62 * 1024 * 1024
            ),
        )(
            *(
                pltpu.with_memory_space_constraint(x, pltpu.HBM)
                for x in (right_side, band_blocks, link_blocks, jnp.transpose(link_rows, (0, 2, 1)))
            )
        )
        return pl.pallas_call(
            mix,
            out_shape=(field, field),
            in_specs=[local_vmem] * 3,
            out_specs=(hbm, hbm),
            scratch_shapes=[vmem(field.shape, F32), vmem(field.shape, F32), dma((2, 2))],
        )(*(pltpu.with_memory_space_constraint(o, pltpu.VMEM) for o in outs))

    return jax.shard_map(
        local,
        mesh=mesh,
        in_specs=(P("dom", None, None), P("dom", None, None, None), P("dom", None, None, None, None), P("dom", None, None)),
        out_specs=(P("dom", None, None), P("dom", None, None)),
        check_vma=False,
    )
```
